32 devices in a mesh: gx: 4 (over x, core), gy: 2 (over y), gz: 4 (over z).
Axes of the slice: x: 2, y: 2, z: 4, core: 2. Of those that a mesh axis runs over, the one named last changes fastest.
Arguments:
- offsets: float32 [4, 2, 4, 16, 3, 128], P('gx', 'gy', 'gz'), may hold values from 0 to 1
- burgers: float32 [4, 2, 4, 16, 3, 128], P('gx', 'gy', 'gz'), may hold values from -2 to 2
- lines: float32 [4, 2, 4, 16, 3, 128], P('gx', 'gy', 'gz'), may hold values from -2 to 2
- pair_list: int32 [2048, 2], P(('gx', 'gy', 'gz')), may hold values from 0 to 431, as said below
- pair_count: int32 [32], P(('gx', 'gy', 'gz')), may hold values from 8 to 64, as said below
Outputs:
- forces: float32 [4, 2, 4, 16, 3, 128], P('gx', 'gy', 'gz')
The draws below stay inside these ranges and needn't reach their ends.
Inputs may be any that keep to these rules, and one draw needn't show every extreme that they name: `pair_list`: column 0 of each row is an own block, under 16; column 1 is k * 16 + b with k of 0 to 26 and b under 16; a row never pairs a block with itself. `pair_count`: some cell has all 64 rows live in every draw.
All inputs are finite; a program needn't handle non-finite values.
Results may differ from the reference program's by a relative error of at most 0.0003.
Values sent between devices are 32-bit elements; how exact they have to be, the bound alone decides.
No kernel may reach another device: no remote copies, remote signals or barrier semaphores. Data moves between devices by JAX's collectives and lax.ppermute only.
A program may use at most 64 MiB of HBM per device.

```python
import math
import jax
import jax.numpy as jnp
import numpy as np
from jax import lax

BLOCK = 128
BLK_DEV = 16
PAIR_DEV = 64
CELLS = 32
N_GX = 4
N_GY = 2
N_GZ = 4


def draw_pair_list(key, part):
    rows = CELLS * PAIR_DEV
    first_key = jax.random.fold_in(key, 11)
    second_key = jax.random.fold_in(key, 12)
    third_key = jax.random.fold_in(key, 13)
    own = jax.random.randint(first_key, (rows,), 0, BLK_DEV)
    cell = jax.random.randint(second_key, (rows,), 0, 27)
    other = jax.random.randint(third_key, (rows,), 0, BLK_DEV)
    clash = (cell == 13) & (other == own)
    other = jnp.where(clash, (own + 1) % BLK_DEV, other)
    return jnp.stack([own, cell * BLK_DEV + other], axis=1).astype(jnp.int32)


def draw_pair_count(key, part):
    first_key = jax.random.fold_in(key, 21)
    second_key = jax.random.fold_in(key, 22)
    halvings = jax.random.randint(first_key, (CELLS,), 0, 4)
    counts = jnp.right_shift(jnp.full((CELLS,), PAIR_DEV, jnp.int32), halvings.astype(jnp.int32))
    chosen = jax.random.randint(second_key, (), 0, CELLS)
    counts = jnp.where(jnp.arange(CELLS) == chosen, PAIR_DEV, counts)
    return counts.astype(jnp.int32)


def block_scale(key, extent, split, smallest, largest):
    loudness, own = 1.0, jax.random.fold_in(key, 6)
    for dim, parts in split:
        heights = jnp.exp(jax.random.uniform(jax.random.fold_in(own, dim), (parts,), jnp.float32, smallest / len(split), largest / len(split)))
        loudness = loudness * jnp.repeat(heights, extent[dim] // parts).reshape([-1 if axis == dim else 1 for axis in range(len(extent))])
    return loudness


def bell_draw(stream_key, shape, scale, limit, shards=(), held_as=jnp.bfloat16):
    values = scale * jax.random.normal(stream_key, shape, jnp.float32)
    if shards:
        values = values * block_scale(stream_key, shape, shards, -0.22, 0.18)
    return jnp.clip(values, -limit, limit).astype(held_as)


def setup_inputs(seed: int = 0) -> dict:
    streams_of = jax.random.split(jax.random.key(seed), 6)
    offsets = jnp.clip(1.0 * jax.random.uniform(streams_of[0], (N_GX, N_GY, N_GZ, BLK_DEV, 3, BLOCK), jnp.float32) ** block_scale(streams_of[0], (N_GX, N_GY, N_GZ, BLK_DEV, 3, BLOCK), ((0, 4), (1, 2), (2, 4)), -0.2, 0.2), 0.0, 1.0)
    burgers = bell_draw(streams_of[1], (N_GX, N_GY, N_GZ, BLK_DEV, 3, BLOCK), 0.35, 2.0, ((0, 4), (1, 2), (2, 4)), jnp.float32)
    lines = bell_draw(streams_of[2], (N_GX, N_GY, N_GZ, BLK_DEV, 3, BLOCK), 0.35, 2.0, ((0, 4), (1, 2), (2, 4)), jnp.float32)
    pair_list = draw_pair_list(jax.random.fold_in(streams_of[5], 71), 0)
    pair_count = draw_pair_count(jax.random.fold_in(streams_of[5], 71), 0)
    return {"offsets": offsets, "burgers": burgers, "lines": lines, "pair_list": pair_list, "pair_count": pair_count}


CORE_SQ = 0.0625

def multi_indices(top):
    result = []
    for order in range(top + 1):
        for i in range(order, -1, -1):
            for j in range(order - i, -1, -1):
                result.append((i, j, order - i - j))
    return result

def expansion_tables():
    low = multi_indices(3)
    high = {m: n for n, m in enumerate(multi_indices(6))}
    index = np.array([[high[b[0] + a[0], b[1] + a[1], b[2] + a[2]] for a in low] for b in low], np.int32)
    signs = np.array([(-1.0) ** sum(a) for a in low], np.float32)
    where_low = {m: n for n, m in enumerate(low)}
    descend = np.array([[where_low[tuple((g[r] + (1 if r == k else 0) for r in range(3)))] for g in low[:10]] for k in range(3)], np.int32)
    return (index, signs, descend)

def potential(point):
    return lax.rsqrt(jnp.sum(point * point) + CORE_SQ)

def partial_of(parent, axis_number):

    def derived(point):
        return jax.grad(parent)(point)[axis_number]
    return derived

def derivative_table(points):
    makers = {(0, 0, 0): potential}
    columns = []
    for index_set in multi_indices(6):
        if index_set not in makers:
            axis_number = [r for r in range(3) if index_set[r] > 0][0]
            lower = tuple((index_set[r] - (1 if r == axis_number else 0) for r in range(3)))
            makers[index_set] = partial_of(makers[lower], axis_number)
        columns.append(jax.vmap(makers[index_set])(points))
    return jnp.stack(columns, axis=1)

def monomials(delta):
    rows = []
    for i, j, k in multi_indices(3):
        scale = 1.0 / (math.factorial(i) * math.factorial(j) * math.factorial(k))
        rows.append(delta[0] ** i * delta[1] ** j * delta[2] ** k * scale)
    return jnp.stack(rows, axis=0)

def cell_moments(delta, strength):
    return jnp.dot(monomials(delta), strength.T, precision=lax.Precision.HIGHEST)

def far_field(table, separation, moments, delta, strength):
    index, signs, descend = expansion_tables()
    distant = (lax.optimization_barrier(jnp.max(jnp.abs(separation), axis=1)) > 1.5).astype(jnp.float32)
    coupling = table[:, index] * signs[None, None, :] * distant[:, None, None]
    local = jnp.einsum('cba,cak->bk', coupling, moments, precision=lax.Precision.HIGHEST)
    projected = jnp.dot(local, strength, precision=lax.Precision.HIGHEST)
    basis = monomials(delta)[:10]
    return -jnp.stack([lax.optimization_barrier(jnp.sum(basis * projected[descend[k]], axis=0)) for k in range(3)], axis=0)

def cross_rows(left, right):
    return jnp.stack([left[..., 1, :] * right[..., 2, :] - left[..., 2, :] * right[..., 1, :], left[..., 2, :] * right[..., 0, :] - left[..., 0, :] * right[..., 2, :], left[..., 0, :] * right[..., 1, :] - left[..., 1, :] * right[..., 0, :]], axis=-2)

def pair_force(target_pos, target_q, source_pos, source_q):
    separation = target_pos[:, :, None] - source_pos[:, None, :]
    inverse = lax.rsqrt(lax.optimization_barrier(jnp.sum(separation * separation, axis=0)) + CORE_SQ)
    cube = inverse * inverse * inverse
    fifth = cube * inverse * inverse
    alike = lax.optimization_barrier(jnp.sum(target_q[:, :, None] * source_q[:, None, :], axis=0))
    along_target = lax.optimization_barrier(jnp.sum(target_q[:, :, None] * separation, axis=0))
    along_source = lax.optimization_barrier(jnp.sum(source_q[:, None, :] * separation, axis=0))
    weight = alike * cube + 3.0 * along_target * along_source * fifth
    field = weight[None] * separation - (along_source * cube)[None] * target_q[:, :, None] - (along_target * cube)[None] * source_q[:, None, :]
    return (lax.optimization_barrier(jnp.sum(field, axis=2)), -lax.optimization_barrier(jnp.sum(field, axis=1)))

def place(flat, blocks):
    cell = jnp.arange(flat.shape[0], dtype=jnp.int32) // blocks
    shift = jnp.stack([cell // 9 - 1, cell // 3 % 3 - 1, cell % 3 - 1], axis=1).astype(jnp.float32)
    return flat.at[:, :3, :].add(shift[:, :, None])

def add_self(hood, totals, blocks):
    own = hood[13 * blocks:14 * blocks]
    on_target, unused = jax.vmap(pair_force)(own[:, :3], own[:, 3:], own[:, :3], own[:, 3:])
    return totals.at[13 * blocks:14 * blocks].add(on_target)

def sweep(hood, pairs, first_pair, last_pair, totals):
    blocks = hood.shape[0] // 27

    def one_group(turn, totals):
        start = turn * 8
        rows = lax.dynamic_slice_in_dim(pairs, start, 8, 0)
        number = start + jnp.arange(8, dtype=jnp.int32)
        live = ((number >= first_pair) & (number < last_pair)).astype(jnp.float32)[:, None, None]
        targets = 13 * blocks + rows[:, 0]
        sources = rows[:, 1]
        target_data = hood[targets]
        source_data = hood[sources]
        on_target, on_source = jax.vmap(pair_force)(target_data[:, :3], target_data[:, 3:], source_data[:, :3], source_data[:, 3:])
        totals = totals.at[targets].add(on_target * live)
        return totals.at[sources].add(on_source * live)
    return lax.fori_loop(first_pair // 8, (last_pair + 7) // 8, one_group, totals)

def reference(offsets, burgers, lines, pair_list, pair_count):
    blocks = BLK_DEV
    cells = N_GX * N_GY * N_GZ
    strength = cross_rows(burgers, lines)
    data = jnp.concatenate([offsets, strength], axis=-2)
    padded = jnp.pad(data, ((1, 1), (1, 1), (1, 1), (0, 0), (0, 0), (0, 0)))
    pairs = pair_list.reshape(cells, PAIR_DEV, 2)
    nought = jnp.zeros((), jnp.int32)

    def one_device(totals, device):
        xpos = device // (N_GY * N_GZ)
        ypos = device // N_GZ % N_GY
        zpos = device % N_GZ
        corner = (xpos, ypos, zpos, nought, nought, nought)
        window = lax.dynamic_slice(padded, corner, (3, 3, 3, blocks, 6, BLOCK)).reshape(27 * blocks, 6, BLOCK)
        hood = place(window, blocks)
        local = jnp.zeros((27 * blocks, 3, BLOCK), jnp.float32)
        local = add_self(hood, local, blocks)
        local = sweep(hood, pairs[device], jnp.zeros((), jnp.int32), pair_count[device], local)
        current = lax.dynamic_slice(totals, corner, (3, 3, 3, blocks, 3, BLOCK))
        totals = lax.dynamic_update_slice(totals, current + local.reshape(3, 3, 3, blocks, 3, BLOCK), corner)
        return (totals, None)
    start = jnp.zeros((N_GX + 2, N_GY + 2, N_GZ + 2, blocks, 3, BLOCK), jnp.float32)
    totals, unused = lax.scan(one_device, start, jnp.arange(cells, dtype=jnp.int32))
    near = totals[1:-1, 1:-1, 1:-1]
    cellwise = jnp.moveaxis(data.reshape(cells, blocks, 6, BLOCK), 2, 1).reshape(cells, 6, blocks * BLOCK)
    deltas = cellwise[:, :3] - 0.5
    strengths = cellwise[:, 3:]
    moments = jax.vmap(cell_moments)(deltas, strengths)
    span_y = 2 * N_GY - 1
    span_z = 2 * N_GZ - 1
    grid_x, grid_y, grid_z = jnp.meshgrid(jnp.arange(-(N_GX - 1), N_GX, dtype=jnp.int32), jnp.arange(-(N_GY - 1), N_GY, dtype=jnp.int32), jnp.arange(-(N_GZ - 1), N_GZ, dtype=jnp.int32), indexing='ij')
    points = jnp.stack([grid_x.reshape(-1), grid_y.reshape(-1), grid_z.reshape(-1)], axis=1).astype(jnp.float32)
    table = derivative_table(points)
    every = jnp.arange(cells, dtype=jnp.int32)
    cell_x = every // (N_GY * N_GZ)
    cell_y = every // N_GZ % N_GY
    cell_z = every % N_GZ

    def one_target(target):
        tx = target // (N_GY * N_GZ)
        ty = target // N_GZ % N_GY
        tz = target % N_GZ
        position = ((tx - cell_x + N_GX - 1) * span_y + (ty - cell_y + N_GY - 1)) * span_z + (tz - cell_z + N_GZ - 1)
        separation = jnp.stack([tx - cell_x, ty - cell_y, tz - cell_z], axis=1).astype(jnp.float32)
        result = far_field(table[position], separation, moments, deltas[target], strengths[target])
        return jnp.moveaxis(result.reshape(3, blocks, BLOCK), 1, 0)
    far = lax.map(one_target, every).reshape(N_GX, N_GY, N_GZ, blocks, 3, BLOCK)
    return near + far
```

```python
import functools
import math

import jax
import jax.numpy as jnp
import numpy as np
from jax import lax
from jax.experimental import pallas as pl
from jax.experimental.pallas import tpu as pltpu
from jax.sharding import PartitionSpec as P

CORE_SQ = 0.0625
AXES = ("gx", "gy", "gz")
LANES = 128
LOW = 20
HIGH = lax.Precision.HIGHEST


def multi_indices(top):
    result = []
    for order in range(top + 1):
        for i in range(order, -1, -1):
            for j in range(order - i, -1, -1):
                result.append((i, j, order - i - j))
    return result


def potential_derivatives(points, top):
    rho = np.sum(points * points, axis=1) + CORE_SQ
    known = {}
    factor = 1.0
    for n in range(top + 1):
        known[(n, 0, 0, 0)] = factor * rho ** (-(n + 0.5))
        factor *= -(2 * n + 1)

    def value(n, index):
        key = (n,) + index
        if key not in known:
            r = [s for s in range(3) if index[s] > 0][0]
            less = list(index)
            less[r] -= 1
            total = points[:, r] * value(n + 1, tuple(less))
            if less[r] > 0:
                lower = list(less)
                lower[r] -= 1
                total = total + less[r] * value(n + 1, tuple(lower))
            known[key] = total
        return known[key]

    return {index: value(0, index) for index in multi_indices(top)}


@functools.lru_cache(maxsize=None)
def coupling_rows(nx, ny, nz):
    grid = np.meshgrid(
        np.arange(-(nx - 1), nx), np.arange(-(ny - 1), ny), np.arange(-(nz - 1), nz), indexing="ij"
    )
    shift = np.stack([g.reshape(-1) for g in grid], axis=1).astype(np.float64)
    table = potential_derivatives(-shift, 6)
    far = (np.max(np.abs(shift), axis=1) > 1.5).astype(np.float64)
    low = multi_indices(3)
    width = -(-LOW * LOW // LANES) * LANES
    rows = np.zeros((shift.shape[0], width), np.float32)
    for a, alpha in enumerate(low):
        for b, beta in enumerate(low):
            index = tuple(alpha[r] + beta[r] for r in range(3))
            rows[:, a * LOW + b] = (-1.0) ** sum(alpha) * table[index] * far
    return rows


def split_const(value, size):
    if size & (size - 1) == 0:
        bits = size.bit_length() - 1
        return jnp.right_shift(value, bits), jnp.bitwise_and(value, size - 1)
    high = lax.div(value, jnp.int32(size))
    return high, value - high * size


def ninths(k):
    nine = jnp.right_shift(k * 57, 9)
    rest = k - 9 * nine
    three = jnp.right_shift(rest * 11, 5)
    return nine - 1, three - 1, rest - 3 * three - 1, rest


def monomial_rows(e):
    rows = []
    for i, j, k in multi_indices(3):
        scale = 1.0 / (math.factorial(i) * math.factorial(j) * math.factorial(k))
        term = None
        for r, power in enumerate((i, j, k)):
            for _ in range(power):
                term = e[r] if term is None else term * e[r]
        if term is None:
            rows.append((None, scale))
        else:
            rows.append((term, scale))
    return rows


def pack_kernel(sizes, blocks, pos_ref, count_ref, pairs_ref, off_ref, bur_ref, lin_ref,
                cell_ref, list_ref, sums_ref, part_ref):
    nx, ny, nz = sizes
    e = [off_ref[:, r, :] - 0.5 for r in range(3)]
    b = [bur_ref[:, r, :] for r in range(3)]
    l = [lin_ref[:, r, :] for r in range(3)]
    q = [b[1] * l[2] - b[2] * l[1], b[2] * l[0] - b[0] * l[2], b[0] * l[1] - b[1] * l[0]]
    for r in range(3):
        cell_ref[r * blocks : (r + 1) * blocks, :] = e[r]
        cell_ref[(3 + r) * blocks : (4 + r) * blocks, :] = q[r]
    rows = pairs_ref.shape[0]
    n = pairs_ref[:, 1:2].astype(jnp.float32)
    a = pairs_ref[:, 0:1].astype(jnp.float32)
    k = jnp.floor((n + 0.5) * (1.0 / blocks))
    nine = jnp.floor((k + 0.5) * (1.0 / 9.0))
    rest = k - 9.0 * nine
    three = jnp.floor((rest + 0.5) * (1.0 / 3.0))
    one = rest - 3.0 * three
    row = lax.broadcasted_iota(jnp.int32, (rows, 1), 0)
    live = row < count_ref[0]
    for digit, axis, size in ((nine, 0, nx), (three, 1, ny), (one, 2, nz)):
        place = digit + (pos_ref[axis] - 1).astype(jnp.float32)
        live = live & (place >= 0.0) & (place < float(size))
    middle = jnp.where(rest == 4.0, 0.0, jnp.where(rest < 4.0, rest + 1.0, rest))
    spot = jnp.where(nine == 1.0, middle, jnp.where(nine == 0.0, 9.0 + rest, 18.0 + rest))
    spot = jnp.where(live, spot, 27.0)
    code = n * float(blocks) + a
    lane = lax.broadcasted_iota(jnp.int32, (rows, LANES), 1)
    down = lax.broadcasted_iota(jnp.int32, (rows, LANES), 0)
    spot_b = jnp.broadcast_to(spot, (rows, LANES))
    code_b = jnp.broadcast_to(code, (rows, LANES))
    spot_row = jnp.sum(jnp.where(lane == down, spot_b, 0.0), axis=0, keepdims=True)
    ahead = (spot_row < spot_b) | ((spot_row == spot_b) & (lane < down))
    rank = jnp.sum(jnp.where(ahead & (lane < rows), 1.0, 0.0), axis=1, keepdims=True)
    lane_f = lane.astype(jnp.float32)
    ordered = jnp.sum(jnp.where(rank == lane_f, code_b, 0.0), axis=0, keepdims=True)
    starts = jnp.sum(
        jnp.where(spot_b < lane_f - float(rows), 1.0, 0.0), axis=0, keepdims=True
    )
    line = jnp.where(lane[:1] < rows, ordered, starts)
    cell_ref[6 * blocks : 6 * blocks + 8, :] = jnp.broadcast_to(line, (8, LANES))
    list_ref[...] = jnp.broadcast_to(line, (8, LANES)).astype(jnp.int32)
    part_ref[...] = jnp.zeros_like(part_ref)
    for m, (term, scale) in enumerate(monomial_rows(e)):
        for r in range(3):
            value = q[r] if term is None else term * q[r]
            line = jnp.sum(value, axis=0, keepdims=True)
            part_ref[r * LOW + m : r * LOW + m + 1, :] = line if scale == 1.0 else line * scale
    turned = part_ref[...].T
    sums_ref[...] = jnp.broadcast_to(jnp.sum(turned, axis=0, keepdims=True), (8, LANES))


def near_sum(blocks, own_ref, sources, job_ref, job_count, acc_ref, scratch):
    yt = scratch[0:2]
    wide = scratch[2:4]
    cells_of = sources[0].shape[0]
    row6 = lax.broadcasted_iota(jnp.int32, (6, LANES), 0)

    def unpack(j):
        high, x = split_const(job_ref[j], blocks)
        high, b = split_const(high, blocks)
        cell, k = split_const(high, 32)
        return x, b, cell, k

    def turn(j, slot):
        x, b, cell, k = unpack(j)
        dx, dy, dz, _ = ninths(k)
        if len(sources) == 1:
            y = sources[0][cell, pl.ds(b, 6, stride=blocks), :]
        else:
            local = jnp.where(cell >= cells_of, cell - cells_of, cell)
            y0 = sources[0][local, pl.ds(b, 6, stride=blocks), :]
            y1 = sources[1][local, pl.ds(b, 6, stride=blocks), :]
            y = jnp.where(cell >= cells_of, y1, y0)
        shift = jnp.where(
            row6 == 0, dx, jnp.where(row6 == 1, dy, jnp.where(row6 == 2, dz, 0))
        ).astype(jnp.float32)
        y = jnp.concatenate([y + shift, jnp.zeros((2, LANES), jnp.float32)], axis=0)
        yt[slot][...] = y.T

    def widen(slot):
        for t in range(LANES // 8):
            tile = yt[slot][8 * t : 8 * t + 8, :]
            for c in range(6):
                wide[slot][6 * t + c] = jnp.broadcast_to(tile[:, c : c + 1], (8, LANES))

    def work(j, slot):
        x, b, cell, k = unpack(j)
        own = [
            jnp.broadcast_to(own_ref[pl.ds(c * blocks + x, 1), :], (8, LANES)) for c in range(6)
        ]
        own3 = [3.0 * own[3 + c] for c in range(3)]
        total = None
        for t in range(LANES // 8):
            y = [wide[slot][6 * t + c] for c in range(6)]
            r = [own[c] - y[c] for c in range(3)]
            square = (r[0] * r[0] + r[1] * r[1]) + (r[2] * r[2] + CORE_SQ)
            s = lax.rsqrt(square)
            s2 = s * s
            s3 = s2 * s
            alike = own[3] * y[3] + own[4] * y[4] + own[5] * y[5]
            u3 = own3[0] * r[0] + own3[1] * r[1] + own3[2] * r[2]
            v = y[3] * r[0] + y[4] * r[1] + y[5] * r[2]
            w = s3 * (alike + (u3 * v) * s2)
            u3s = u3 * s3
            terms = [w * r[0], w * r[1], w * r[2], u3s * y[3], u3s * y[4], u3s * y[5], v * s3]
            total = terms if total is None else [p + n for p, n in zip(total, terms)]
        for c in range(7):
            acc_ref[7 * x + c] += total[c]

    @pl.when(job_count > 0)
    def _():
        last = job_count - 1
        turn(0, 0)
        turn(jnp.minimum(1, last), 1)
        widen(0)

        def pair(i, carry):
            j = 2 * i
            widen(1)
            turn(jnp.minimum(j + 2, last), 0)
            work(j, 0)
            widen(0)
            turn(jnp.minimum(j + 3, last), 1)

            work(j + 1, 1)
            return carry

        lax.fori_loop(0, job_count // 2, pair, 0)

        @pl.when(job_count % 2 == 1)
        def _():
            work(last, 0)


def put_jobs(job_ref, count, list_ref, row, begin, end, entry):
    def one(r, count):
        job_ref[count] = entry(list_ref[row, r])
        return count + 1

    return lax.fori_loop(begin, end, one, count)


def finish_near(blocks, own_ref, acc_ref):
    out = [[], [], []]
    for x in range(blocks):
        sums = [jnp.sum(acc_ref[7 * x + c], axis=0, keepdims=True) for c in range(7)]
        for r in range(3):
            q = own_ref[(3 + r) * blocks + x : (3 + r) * blocks + x + 1, :]
            out[r].append(sums[r] - sums[3 + r] * (1.0 / 3.0) - q * sums[6])
    return [jnp.concatenate(o, axis=0) for o in out]


def slot_of(delta, size):
    if size == 2:
        return jnp.abs(delta)
    return jnp.where(delta < 0, 1, jnp.where(delta > 0, 2, 0))


def slot_delta(slot, size, place):
    if slot == 0:
        return jnp.int32(0)
    if size == 2:
        return 1 - 2 * place
    return jnp.int32(-1 if slot == 1 else 1)


def own_entry(blocks, sizes, slots, base, code):
    n, a = split_const(code, blocks)
    k, b = split_const(n, blocks)
    dx, dy, dz, _ = ninths(k)
    cell = slot_of(dz, sizes[2]) * slots[1] + slot_of(dy, sizes[1])
    cell = cell + base(dx)
    return ((cell * 32 + k) * blocks + b) * blocks + a


def their_entry(blocks, cell, k, code):
    n, a = split_const(code, blocks)
    _, b = split_const(n, blocks)
    return ((cell * 32 + k) * blocks + a) * blocks + b


def near_kernel(stage, sizes, slots, blocks, rows, pos_ref, list_ref, own_ref, *refs):
    count_src = 2 if stage == 2 else 1
    sources = refs[:count_src]
    force_ref, acc_ref, job_ref, ints_ref, lists_ref, sem = refs[count_src : count_src + 6]
    scratch = refs[count_src + 6 :]
    acc_ref[...] = jnp.zeros_like(acc_ref)
    per = slots[1] * slots[2]
    if stage > 0:
        for s, source in enumerate(sources):
            for c in range(source.shape[0]):
                line = source[c, 6 * blocks : 6 * blocks + 8, :]
                at = (s * source.shape[0] + c) * 8
                ints_ref[at : at + 8, :] = line.astype(jnp.int32)
        copy = pltpu.make_async_copy(ints_ref, lists_ref, sem)
        copy.start()
    begin = {0: 0, 1: 1, 2: 9}[stage]
    end = {0: 1, 1: 9, 2: 27}[stage]

    def base(dx):
        if stage == 2:
            return jnp.where(dx > 0, per, 0)
        return 0

    count = jnp.int32(0)
    if stage == 0:
        def self_job(x, count):
            job_ref[count] = (13 * blocks + x) * blocks + x
            return count + 1

        count = lax.fori_loop(0, blocks, self_job, count)
    count = put_jobs(
        job_ref, count, list_ref, 0, list_ref[0, rows + begin], list_ref[0, rows + end],
        functools.partial(own_entry, blocks, sizes, slots, base),
    )
    if stage == 0:
        count = put_jobs(
            job_ref, count, list_ref, 0, list_ref[0, rows], list_ref[0, rows + 1],
            functools.partial(their_entry, blocks, 0, 13),
        )
    else:
        copy.wait()
        for side in range(count_src):
            dx = jnp.int32(0 if stage == 1 else 2 * side - 1)
            for sz in range(slots[2]):
                for sy in range(slots[1]):
                    cell = sz * slots[1] + sy
                    if stage == 1 and cell == 0:
                        continue
                    dy = slot_delta(sy, sizes[1], pos_ref[1])
                    dz = slot_delta(sz, sizes[2], pos_ref[2])
                    k = 9 * (dx + 1) + 3 * (dy + 1) + dz + 1
                    rest = 26 - k - 9 * (1 - dx)
                    if stage == 1:
                        spot = jnp.where(rest < 4, rest + 1, rest)
                    elif side == 0:
                        spot = 18 + rest
                    else:
                        spot = 9 + rest
                    at = (side * per + cell) * 8
                    count = put_jobs(
                        job_ref, count, lists_ref, at,
                        lists_ref[at, rows + spot], lists_ref[at, rows + spot + 1],
                        functools.partial(their_entry, blocks, side * per + cell, k),
                    )
    near_sum(blocks, own_ref, sources, job_ref, count, acc_ref, scratch)
    force = finish_near(blocks, own_ref, acc_ref)
    for r in range(3):
        force_ref[r * blocks : (r + 1) * blocks, :] = force[r]


def far_kernel(blocks, own_ref, sums_ref, table_ref, *refs):
    parts, out_ref = refs[:-1], refs[-1]
    width = table_ref.shape[1]
    every = lax.dot_general(
        sums_ref[...], table_ref[...], (((0,), (0,)), ((), ())),
        precision=HIGH, preferred_element_type=jnp.float32,
    )
    row = lax.broadcasted_iota(jnp.int32, (LANES, width), 0).astype(jnp.float32)
    col = lax.broadcasted_iota(jnp.int32, (LANES, width), 1).astype(jnp.float32)
    alpha = row - LOW * jnp.floor((row + 0.5) * (1.0 / LOW))
    every = jnp.where(alpha == jnp.floor((col + 0.5) * (1.0 / LOW)), every, 0.0)
    pick = (
        jnp.floor((lax.broadcasted_iota(jnp.int32, (8, LANES), 1).astype(jnp.float32) + 0.5) * (1.0 / LOW))
        == lax.broadcasted_iota(jnp.int32, (8, LANES), 0).astype(jnp.float32)
    ).astype(jnp.float32)
    summed = jnp.dot(pick, every, precision=HIGH, preferred_element_type=jnp.float32)
    down = lax.broadcasted_iota(jnp.int32, (width, LANES), 0).astype(jnp.float32)
    beta = down - LOW * jnp.floor((down + 0.5) * (1.0 / LOW))
    fold = (beta == lax.broadcasted_iota(jnp.int32, (width, LANES), 1).astype(jnp.float32)).astype(
        jnp.float32
    )
    local = jnp.dot(summed, fold, precision=HIGH, preferred_element_type=jnp.float32)
    e = [own_ref[r * blocks : (r + 1) * blocks, :] for r in range(3)]
    q = [own_ref[(3 + r) * blocks : (4 + r) * blocks, :] for r in range(3)]
    low = multi_indices(3)
    where_low = {m: n for n, m in enumerate(low)}
    first = low[:10]
    projected = [
        sum(
            q[d] * jnp.broadcast_to(local[d : d + 1, m : m + 1], q[d].shape) for d in range(3)
        )
        for m in range(LOW)
    ]
    basis = monomial_rows(e)[:10]
    for r in range(3):
        far = None
        for g, (term, scale) in zip(first, basis):
            up = tuple(g[s] + (1 if s == r else 0) for s in range(3))
            value = projected[where_low[up]]
            if scale != 1.0:
                value = value * scale
            if term is not None:
                value = value * term
            far = value if far is None else far + value
        total = -far
        for part in parts:
            total = total + part[r * blocks : (r + 1) * blocks, :]
        out_ref[:, r, :] = total


def shift_by(value, axis, distance):
    count = lax.axis_size(axis)
    if distance > 0:
        route = [(i, i + distance) for i in range(count - distance)]
    else:
        route = [(i - distance, i) for i in range(count + distance)]
    return lax.ppermute(value, axis, route)


def neighbours(value, axis):
    count = lax.axis_size(axis)
    if count == 1:
        return []
    if count == 2:
        return [lax.ppermute(value, axis, [(0, 1), (1, 0)])]
    return [shift_by(value, axis, 1), shift_by(value, axis, -1)]


def cyclic(value, axis):
    count = lax.axis_size(axis)
    turns = [
        lax.ppermute(value, axis, [((i + s) % count, i) for i in range(count)])
        for s in range(1, count)
    ]
    return jnp.concatenate([value] + turns, axis=0)


VMEM = pl.BlockSpec(memory_space=pltpu.VMEM)
SMEM = pl.BlockSpec(memory_space=pltpu.SMEM)


def params(mib):
    return pltpu.CompilerParams(vmem_limit_bytes=mib * 1024 * 1024)


def per_device(offsets, burgers, lines, pair_list, pair_count):
    blocks = offsets.shape[3]
    width = offsets.shape[5]
    sizes = tuple(lax.axis_size(a) for a in AXES)
    place = [lax.axis_index(a).astype(jnp.int32) for a in AXES]
    pos = jnp.stack(place)
    rows = pair_list.shape[0]
    own = offsets[0, 0, 0]
    cell_rows = 6 * blocks + 8
    cell, line, sums = pl.pallas_call(
        functools.partial(pack_kernel, sizes, blocks),
        out_shape=(
            jax.ShapeDtypeStruct((cell_rows, width), jnp.float32),
            jax.ShapeDtypeStruct((8, width), jnp.int32),
            jax.ShapeDtypeStruct((8, width), jnp.float32),
        ),
        in_specs=[SMEM, SMEM, VMEM, VMEM, VMEM, VMEM],
        out_specs=(VMEM, VMEM, VMEM),
        scratch_shapes=[pltpu.VMEM((LANES, LANES), jnp.float32)],
        compiler_params=params(4),
        name="pack",
    )(pos, pair_count, pair_list, own, burgers[0, 0, 0], lines[0, 0, 0])

    slots = tuple(min(s, 3) for s in sizes)

    def near(stage, sources):
        total_cells = sum(s.shape[0] for s in sources)
        jobs = blocks + 2 * rows + total_cells * rows
        return pl.pallas_call(
            functools.partial(near_kernel, stage, sizes, slots, blocks, rows),
            out_shape=jax.ShapeDtypeStruct((3 * blocks, width), jnp.float32),
            in_specs=[SMEM, SMEM] + [VMEM] * (1 + len(sources)),
            out_specs=VMEM,
            scratch_shapes=[
                pltpu.VMEM((7 * blocks, 8, LANES), jnp.float32),
                pltpu.SMEM((jobs,), jnp.int32),
                pltpu.VMEM((8 * total_cells, LANES), jnp.int32),
                pltpu.SMEM((8 * total_cells, LANES), jnp.int32),
                pltpu.SemaphoreType.DMA,
                pltpu.VMEM((LANES, 8), jnp.float32),
                pltpu.VMEM((LANES, 8), jnp.float32),
                pltpu.VMEM((6 * LANES // 8, 8, LANES), jnp.float32),
                pltpu.VMEM((6 * LANES // 8, 8, LANES), jnp.float32),
            ],
            compiler_params=params(16),
            name="near%d" % stage,
        )(pos, line, cell, *sources)

    level = cell[None]
    level = jnp.concatenate([level] + neighbours(level, "gy"), axis=0)
    near0 = near(0, [cell[None]])
    level = jnp.concatenate([level] + neighbours(level, "gz"), axis=0)
    sides = neighbours(level, "gx")
    near1 = near(1, [level])
    near2 = near(2, sides)

    moments = sums[:1]
    for axis in ("gy", "gz", "gx"):
        moments = cyclic(moments, axis)
    ranges = [(place[a] + jnp.arange(sizes[a], dtype=jnp.int32)) % sizes[a] - place[a] for a in range(3)]
    ranges = [ranges[a] + (sizes[a] - 1) for a in range(3)]
    number = (
        (ranges[0][:, None, None] * (2 * sizes[1] - 1) + ranges[1][None, None, :])
        * (2 * sizes[2] - 1)
        + ranges[2][None, :, None]
    ).reshape(-1)
    table = jnp.take(jnp.asarray(coupling_rows(*sizes)), number, axis=0)
    forces = pl.pallas_call(
        functools.partial(far_kernel, blocks),
        out_shape=jax.ShapeDtypeStruct(own.shape, jnp.float32),
        in_specs=[VMEM] * 6,
        out_specs=VMEM,
        compiler_params=params(16),
        name="far",
    )(cell, moments, table, near0, near1, near2)
    return forces[None, None, None]


def solution(mesh):
    return jax.shard_map(
        per_device,
        mesh=mesh,
        in_specs=(
            P("gx", "gy", "gz", None, None, None),
            P("gx", "gy", "gz", None, None, None),
            P("gx", "gy", "gz", None, None, None),
            P(("gx", "gy", "gz"), None),
            P(("gx", "gy", "gz")),
        ),
        out_specs=P("gx", "gy", "gz", None, None, None),
        check_vma=False,
    )
```

```python
import functools
import math

import jax
import jax.numpy as jnp
import numpy as np
from jax import lax
from jax.experimental import pallas as pl
from jax.experimental.pallas import tpu as pltpu
from jax.sharding import PartitionSpec as P

CORE_SQ = 0.0625
AXES = ("gx", "gy", "gz")
LANES = 128
COST = (int(1e9), int(1e9), int(3e9), int(5e8))
LOW = 20
HIGH = lax.Precision.HIGHEST


def multi_indices(top):
    result = []
    for order in range(top + 1):
        for i in range(order, -1, -1):
            for j in range(order - i, -1, -1):
                result.append((i, j, order - i - j))
    return result


def potential_derivatives(points, top):
    rho = np.sum(points * points, axis=1) + CORE_SQ
    known = {}
    factor = 1.0
    for n in range(top + 1):
        known[(n, 0, 0, 0)] = factor * rho ** (-(n + 0.5))
        factor *= -(2 * n + 1)

    def value(n, index):
        key = (n,) + index
        if key not in known:
            r = [s for s in range(3) if index[s] > 0][0]
            less = list(index)
            less[r] -= 1
            total = points[:, r] * value(n + 1, tuple(less))
            if less[r] > 0:
                lower = list(less)
                lower[r] -= 1
                total = total + less[r] * value(n + 1, tuple(lower))
            known[key] = total
        return known[key]

    return {index: value(0, index) for index in multi_indices(top)}


@functools.lru_cache(maxsize=None)
def coupling_rows(nx, ny, nz):
    grid = np.meshgrid(
        np.arange(-(nx - 1), nx), np.arange(-(ny - 1), ny), np.arange(-(nz - 1), nz), indexing="ij"
    )
    shift = np.stack([g.reshape(-1) for g in grid], axis=1).astype(np.float64)
    table = potential_derivatives(-shift, 6)
    far = (np.max(np.abs(shift), axis=1) > 1.5).astype(np.float64)
    low = multi_indices(3)
    width = -(-LOW * LOW // LANES) * LANES
    rows = np.zeros((shift.shape[0], width), np.float32)
    for a, alpha in enumerate(low):
        for b, beta in enumerate(low):
            index = tuple(alpha[r] + beta[r] for r in range(3))
            rows[:, a * LOW + b] = (-1.0) ** sum(alpha) * table[index] * far
    return rows


def split_const(value, size):
    if size & (size - 1) == 0:
        bits = size.bit_length() - 1
        return jnp.right_shift(value, bits), jnp.bitwise_and(value, size - 1)
    high = lax.div(value, jnp.int32(size))
    return high, value - high * size


def ninths(k):
    nine = jnp.right_shift(k * 57, 9)
    rest = k - 9 * nine
    three = jnp.right_shift(rest * 11, 5)
    return nine - 1, three - 1, rest - 3 * three - 1, rest


def monomial_rows(e):
    rows = []
    for i, j, k in multi_indices(3):
        scale = 1.0 / (math.factorial(i) * math.factorial(j) * math.factorial(k))
        term = None
        for r, power in enumerate((i, j, k)):
            for _ in range(power):
                term = e[r] if term is None else term * e[r]
        if term is None:
            rows.append((None, scale))
        else:
            rows.append((term, scale))
    return rows


def pack_kernel(sizes, slots, blocks, pos_ref, count_ref, pairs_ref, off_any, bur_any, lin_any,
                cell_ref, list_ref, part_ref, off_ref, bur_ref, lin_ref, sems):
    copies = [
        pltpu.make_async_copy(source, target, sems.at[n])
        for n, (source, target) in enumerate(
            ((off_any, off_ref), (bur_any, bur_ref), (lin_any, lin_ref))
        )
    ]
    for copy in copies:
        copy.start()
    part_ref[...] = jnp.zeros_like(part_ref)
    rows = pairs_ref.shape[1]
    n = pairs_ref[1:2, :].astype(jnp.float32)
    a = pairs_ref[0:1, :].astype(jnp.float32)
    k = jnp.floor((n + 0.5) * (1.0 / blocks))
    nine = jnp.floor((k + 0.5) * (1.0 / 9.0))
    rest = k - 9.0 * nine
    three = jnp.floor((rest + 0.5) * (1.0 / 3.0))
    one = rest - 3.0 * three
    live = lax.broadcasted_iota(jnp.int32, (1, rows), 1) < count_ref[...]
    for digit, axis in ((nine, 0), (three, 1), (one, 2)):
        where = digit + (pos_ref[:, axis : axis + 1] - 1).astype(jnp.float32)
        live = live & (where >= 0.0) & (where < float(sizes[axis]))
    middle = jnp.where(rest == 4.0, 0.0, jnp.where(rest < 4.0, rest + 1.0, rest))
    spot = jnp.where(nine == 1.0, middle, jnp.where(nine == 0.0, 9.0 + rest, 18.0 + rest))
    spot = jnp.where(live, spot, 27.0)
    code = n * float(blocks) + a
    cell = jnp.zeros_like(n)
    for digit, axis, weight in ((one, 2, slots[1]), (three, 1, 1), (nine, 0, slots[1] * slots[2])):
        first = (1 - 2 * jnp.bitwise_and(pos_ref[:, axis : axis + 1], 1)).astype(jnp.float32)
        slot = jnp.where(digit == 1.0, 0.0, jnp.where(digit - 1.0 == first, 1.0, 2.0))
        cell = cell + float(weight) * (jnp.maximum(slot - 1.0, 0.0) if axis == 0 else slot)
    job = ((cell * 32.0 + k) * float(blocks) + n - float(blocks) * k) * float(blocks) + a
    lane = lax.broadcasted_iota(jnp.int32, (rows, rows), 1)
    down = lax.broadcasted_iota(jnp.int32, (rows, rows), 0)
    spot_c = jnp.sum(jnp.where(lane == down, spot, 0.0), axis=1, keepdims=True)
    code_c = jnp.sum(jnp.where(lane == down, code, 0.0), axis=1, keepdims=True)
    job_c = jnp.sum(jnp.where(lane == down, job, 0.0), axis=1, keepdims=True)
    ahead = (spot < spot_c) | ((spot == spot_c) & (lane < down))
    rank = jnp.sum(jnp.where(ahead, 1.0, 0.0), axis=1, keepdims=True)
    lane_f = lax.broadcasted_iota(jnp.int32, (rows, LANES), 1).astype(jnp.float32)
    ordered = jnp.sum(jnp.where(rank == lane_f, code_c, 0.0), axis=0, keepdims=True)
    jobs = jnp.sum(jnp.where(rank == lane_f, job_c, 0.0), axis=0, keepdims=True)
    starts = jnp.sum(jnp.where(spot_c < lane_f - float(rows), 1.0, 0.0), axis=0, keepdims=True)
    line = jnp.where(lane_f[:1] < float(rows), ordered, starts)
    cell_ref[6 * blocks : 6 * blocks + 8, :] = jnp.broadcast_to(line, (8, LANES))
    line = jnp.where(lane_f[:1] < float(rows), jobs, starts)
    list_ref[...] = jnp.broadcast_to(line, (8, LANES)).astype(jnp.int32)
    for copy in copies:
        copy.wait()
    e = [off_ref[r] - 0.5 for r in range(3)]
    b = [bur_ref[r] for r in range(3)]
    l = [lin_ref[r] for r in range(3)]
    q = [b[1] * l[2] - b[2] * l[1], b[2] * l[0] - b[0] * l[2], b[0] * l[1] - b[1] * l[0]]
    for r in range(3):
        cell_ref[r * blocks : (r + 1) * blocks, :] = e[r]
        cell_ref[(3 + r) * blocks : (4 + r) * blocks, :] = q[r]
    for m, (term, scale) in enumerate(monomial_rows(e)):
        for r in range(3):
            value = q[r] if term is None else term * q[r]
            line = jnp.sum(value, axis=0, keepdims=True)
            part_ref[r * LOW + m : r * LOW + m + 1, :] = line if scale == 1.0 else line * scale
    turned = part_ref[...].T
    cell_ref[6 * blocks + 1 : 6 * blocks + 2, :] = jnp.sum(turned, axis=0, keepdims=True)


def couple_kernel(sizes, pos_ref, all_ref, out_ref):
    def one(s, carry):
        sx, rest = split_const(s, sizes[1] * sizes[2])
        sz, sy = split_const(rest, sizes[1])
        at = jnp.int32(0)
        for axis, slot in ((0, sx), (1, sy), (2, sz)):
            there = jnp.bitwise_xor(pos_ref[axis], slot)
            at = at * (2 * sizes[axis] - 1) + there - pos_ref[axis] + sizes[axis] - 1
        out_ref[pl.ds(s, 1), :] = all_ref[pl.ds(at, 1), :]
        return carry

    lax.fori_loop(0, out_ref.shape[0], one, 0)


def thirds(value):
    first = value.astype(jnp.bfloat16).astype(jnp.float32)
    left = value - first
    second = left.astype(jnp.bfloat16).astype(jnp.float32)
    return first, second, left - second


def weight_kernel(blocks, own_ref, out_ref):
    row = lax.broadcasted_iota(jnp.int32, (8, LANES), 0)

    def one(x, carry):
        own = [
            jnp.broadcast_to(own_ref[pl.ds(c * blocks + x, 1), :], (8, LANES)) for c in range(6)
        ]
        m, q = own[:3], own[3:]
        zero = jnp.zeros((8, LANES), jnp.float32)

        def form(entries):
            total = zero
            for at, value in entries:
                total = jnp.where(row == at, value, total)
            return total

        q3 = [3.0 * c for c in q]
        product = q3[0] * m[0] + q3[1] * m[1] + q3[2] * m[2]
        forms = [form([(r, -1.0), (7, m[r])]) for r in range(3)]
        forms.append(form([(3 + r, q[r]) for r in range(3)]))
        forms.append(form([(r, -q3[r]) for r in range(3)] + [(7, product)]))
        forms.append(form([(3 + r, m[r]) for r in range(3)] + [(6, -1.0)]))
        forms += [form([(3 + r, 1.0)]) for r in range(3)]
        for o, value in enumerate(forms):
            p = thirds(value)
            stacked = jnp.concatenate([p[0], p[1], p[2], p[0], p[1], p[0]], axis=0)
            out_ref[x, :, o * LANES : (o + 1) * LANES] = stacked.astype(jnp.bfloat16)
        return carry

    lax.fori_loop(0, blocks, one, 0)


FORMS = 9


def near_sum(blocks, weight_ref, sources, job_ref, job_count, acc_ref, scratch):
    left = scratch[0:2]
    wide = scratch[2:4]
    cells_of = sources[0].shape[0]
    row6 = lax.broadcasted_iota(jnp.int32, (6, LANES), 0)

    def unpack(j):
        high, x = split_const(job_ref[j], blocks)
        high, b = split_const(high, blocks)
        cell, k = split_const(high, 32)
        return x, b, cell, k

    def turn(j, slot):
        x, b, cell, k = unpack(j)
        dx, dy, dz, _ = ninths(k)
        if len(sources) == 1:
            y = sources[0][cell, pl.ds(b, 6, stride=blocks), :]
        else:
            local = jnp.where(cell >= cells_of, cell - cells_of, cell)
            y0 = sources[0][local, pl.ds(b, 6, stride=blocks), :]
            y1 = sources[1][local, pl.ds(b, 6, stride=blocks), :]
            y = jnp.where(cell >= cells_of, y1, y0)
        shift = jnp.where(
            row6 == 0, dx, jnp.where(row6 == 1, dy, jnp.where(row6 == 2, dz, 0))
        ).astype(jnp.float32)
        y = y + shift
        product = jnp.sum(y[0:3] * y[3:6], axis=0, keepdims=True)
        y = jnp.concatenate([y, product, jnp.ones((1, LANES), jnp.float32)], axis=0)
        p = thirds(y)
        stacked = jnp.concatenate([p[0], p[0], p[0], p[1], p[1], p[2]], axis=0)
        left[slot][...] = stacked.T.astype(jnp.bfloat16)

    def widen(j, slot):
        x = unpack(j)[0]
        wide[slot][...] = jnp.dot(
            left[slot][...], weight_ref[x], preferred_element_type=jnp.float32
        )

    def work(j, slot):
        x = unpack(j)[0]
        total = None
        for t in range(LANES // 8):
            f = [
                wide[slot][8 * t : 8 * t + 8, o * LANES : (o + 1) * LANES] for o in range(FORMS)
            ]
            r, alike, u3, v, q = f[:3], f[3], f[4], f[5], f[6:]
            square = (r[0] * r[0] + r[1] * r[1]) + (r[2] * r[2] + CORE_SQ)
            s = lax.rsqrt(square)
            s2 = s * s
            s3 = s2 * s
            w = s3 * (alike + (u3 * v) * s2)
            u3s = u3 * s3
            terms = [w * r[0], w * r[1], w * r[2], u3s * q[0], u3s * q[1], u3s * q[2], v * s3]
            total = terms if total is None else [p + n for p, n in zip(total, terms)]
        for c in range(7):
            acc_ref[7 * x + c] += total[c]

    @pl.when(job_count > 0)
    def _():
        last = job_count - 1
        turn(0, 0)
        turn(jnp.minimum(1, last), 1)
        widen(0, 0)

        def pair(i, carry):
            j = 2 * i
            third = jnp.minimum(j + 2, last)
            widen(j + 1, 1)
            turn(third, 0)
            work(j, 0)
            widen(third, 0)
            turn(jnp.minimum(j + 3, last), 1)
            work(j + 1, 1)
            return carry

        lax.fori_loop(0, job_count // 2, pair, 0)

        @pl.when(job_count % 2 == 1)
        def _():
            work(last, 0)


def put_jobs(job_ref, count, list_ref, row, begin, end):
    def one(r, count):
        job_ref[count] = list_ref[row, r]
        return count + 1

    return lax.fori_loop(begin, end, one, count)


def near_forces(blocks, own_ref, acc_ref):
    out = [[], [], []]
    for x in range(blocks):
        sums = [jnp.sum(acc_ref[7 * x + c], axis=0, keepdims=True) for c in range(7)]
        for r in range(3):
            q = own_ref[(3 + r) * blocks + x : (3 + r) * blocks + x + 1, :]
            out[r].append(sums[r] - sums[3 + r] * (1.0 / 3.0) - q * sums[6])
    return [jnp.concatenate(o, axis=0) for o in out]


def slot_delta(slot, place):
    if slot == 0:
        return jnp.int32(0)
    first = 1 - 2 * jnp.bitwise_and(place, 1)
    return first if slot == 1 else -first


def near_kernel(stage, slots, blocks, rows, pos_ref, list_ref, weight_ref, *refs):
    scratch = refs[-4:]
    job_ref, ints_ref, lists_ref, sem = refs[-8:-4]
    if stage == 0:
        own_ref, acc_ref = refs[:2]
        sources = [own_ref]
        acc_ref[...] = jnp.zeros_like(acc_ref)
    elif stage == 1:
        sources = [refs[0]]
        before_ref, acc_ref = refs[1:3]
    else:
        sources = refs[:-13]
        before_ref, own_ref, local_ref, out_ref, acc_ref = refs[-13:-8]
    per = slots[1] * slots[2]
    begin = {0: 0, 1: 1, 2: 9}[stage]
    end = {0: 1, 1: 9, 2: 27}[stage]
    bits = blocks.bit_length() - 1
    lane = lax.broadcasted_iota(jnp.int32, (1, LANES), 1)
    theirs = []
    for side, source in enumerate(sources):
        for cell in range(source.shape[0]):
            if stage == 1 and cell == 0:
                continue
            row = len(theirs)
            dx = slot_delta(side + 1 if stage == 2 else 0, pos_ref[0])
            dy = slot_delta(cell % slots[1], pos_ref[1])
            dz = slot_delta(cell // slots[1], pos_ref[2])
            k = 9 * (dx + 1) + 3 * (dy + 1) + dz + 1
            rest = 3 * (1 - dy) + 1 - dz
            if stage == 0:
                spot = jnp.int32(0)
            elif stage == 1:
                spot = jnp.where(rest < 4, rest + 1, rest)
            else:
                spot = jnp.where(dx < 0, 18, 9) + rest
            at = 6 * blocks
            code = source[cell, at : at + 1, :].astype(jnp.int32)
            a = jnp.bitwise_and(code, blocks - 1)
            b = jnp.bitwise_and(jnp.right_shift(code, bits), blocks - 1)
            turned = jnp.left_shift(a, bits) + b + ((side * per + cell) * 32 + k) * (blocks * blocks)
            ints_ref[row : row + 1, :] = jnp.where(lane < rows, turned, code)
            theirs.append((row, spot))
    copy = pltpu.make_async_copy(ints_ref, lists_ref, sem)
    copy.start()
    if stage > 0:
        acc_ref[...] = before_ref[...]
    count = jnp.int32(0)
    if stage == 0:
        def self_job(x, count):
            job_ref[count] = (13 * blocks + x) * blocks + x
            return count + 1

        count = lax.fori_loop(0, blocks, self_job, count)
    count = put_jobs(
        job_ref, count, list_ref, 0, list_ref[0, rows + begin], list_ref[0, rows + end]
    )
    copy.wait()
    for row, spot in theirs:
        count = put_jobs(
            job_ref, count, lists_ref, row,
            lists_ref[row, rows + spot], lists_ref[row, rows + spot + 1],
        )
    near_sum(blocks, weight_ref, sources, job_ref, count, acc_ref, scratch)
    if stage == 2:
        near = near_forces(blocks, own_ref, acc_ref)
        far = far_forces(blocks, own_ref, local_ref[...])
        for r in range(3):
            out_ref[r] = near[r] + far[r]


def local_kernel(table_ref, *refs):
    parts, out_ref = refs[:-1], refs[-1]
    width = table_ref.shape[1]
    every, at = None, 0
    for part in parts:
        value = lax.dot_general(
            part[...], table_ref[at : at + part.shape[0], :], (((0,), (0,)), ((), ())),
            precision=HIGH, preferred_element_type=jnp.float32,
        )
        every = value if every is None else every + value
        at += part.shape[0]
    row = lax.broadcasted_iota(jnp.int32, (LANES, width), 0).astype(jnp.float32)
    col = lax.broadcasted_iota(jnp.int32, (LANES, width), 1).astype(jnp.float32)
    alpha = row - LOW * jnp.floor((row + 0.5) * (1.0 / LOW))
    every = jnp.where(alpha == jnp.floor((col + 0.5) * (1.0 / LOW)), every, 0.0)
    right = lax.broadcasted_iota(jnp.int32, (8, LANES), 1).astype(jnp.float32)
    down = lax.broadcasted_iota(jnp.int32, (8, LANES), 0).astype(jnp.float32)
    pick = (jnp.floor((right + 0.5) * (1.0 / LOW)) == down).astype(jnp.float32)
    summed = jnp.dot(pick, every, precision=HIGH, preferred_element_type=jnp.float32)
    down = lax.broadcasted_iota(jnp.int32, (width, LANES), 0).astype(jnp.float32)
    right = lax.broadcasted_iota(jnp.int32, (width, LANES), 1).astype(jnp.float32)
    beta = down - LOW * jnp.floor((down + 0.5) * (1.0 / LOW))
    fold = (beta == right).astype(jnp.float32)
    out_ref[...] = jnp.dot(summed, fold, precision=HIGH, preferred_element_type=jnp.float32)


def far_forces(blocks, own_ref, local):
    e = [own_ref[r * blocks : (r + 1) * blocks, :] for r in range(3)]
    q = [own_ref[(3 + r) * blocks : (4 + r) * blocks, :] for r in range(3)]
    low = multi_indices(3)
    where_low = {m: n for n, m in enumerate(low)}
    projected = [
        sum(q[d] * jnp.broadcast_to(local[d : d + 1, m : m + 1], q[d].shape) for d in range(3))
        for m in range(LOW)
    ]
    out = []
    for r in range(3):
        far = None
        for g, (term, scale) in zip(low[:10], monomial_rows(e)[:10]):
            up = tuple(g[s] + (1 if s == r else 0) for s in range(3))
            value = projected[where_low[up]]
            if scale != 1.0:
                value = value * scale
            if term is not None:
                value = value * term
            far = value if far is None else far + value
        out.append(-far)
    return out


def joined(first, second):
    rest = [(0, 0)] * (first.ndim - 1)
    above = jnp.pad(first, [(0, second.shape[0])] + rest)
    return above + jnp.pad(second, [(first.shape[0], 0)] + rest)


def neighbours(value, axis):
    count = lax.axis_size(axis)
    found = []
    for first in range(min(count - 1, 2)):
        route = []
        for i in range(first, count - 1, 2):
            route += [(i, i + 1), (i + 1, i)]
        found.append(lax.ppermute(value, axis, route))
    return found


def crossed(value, axis, step):
    return lax.ppermute(value, axis, [(i, i ^ step) for i in range(lax.axis_size(axis))])


HBM = pl.BlockSpec(memory_space=pltpu.HBM)
VMEM = pl.BlockSpec(memory_space=pltpu.VMEM)
SMEM = pl.BlockSpec(memory_space=pltpu.SMEM)


def cost(flops):
    return pl.CostEstimate(flops=flops, bytes_accessed=1 << 20, transcendentals=0)


def params(mib):
    return pltpu.CompilerParams(vmem_limit_bytes=mib * 1024 * 1024)


def per_device(offsets, burgers, lines, pair_list, pair_count):
    blocks = offsets.shape[3]
    width = offsets.shape[5]
    sizes = tuple(lax.axis_size(a) for a in AXES)
    place = [lax.axis_index(a).astype(jnp.int32) for a in AXES]
    pos = jnp.stack(place)
    rows = pair_list.shape[0]
    for size in sizes:
        assert size & (size - 1) == 0
    own, bur, lin = (jnp.swapaxes(v[0, 0, 0], 0, 1) for v in (offsets, burgers, lines))
    cell_rows = 6 * blocks + 8
    slots = tuple(min(s, 3) for s in sizes)
    part = pltpu.VMEM(own.shape, jnp.float32)
    with jax.named_scope("packing"):
        cell, line = pl.pallas_call(
            functools.partial(pack_kernel, sizes, slots, blocks),
            out_shape=(
                jax.ShapeDtypeStruct((cell_rows, width), jnp.float32),
                jax.ShapeDtypeStruct((8, width), jnp.int32),
            ),
            in_specs=[VMEM] * 3 + [HBM] * 3,
            out_specs=(VMEM, VMEM),
            scratch_shapes=[
                pltpu.VMEM((LANES, LANES), jnp.float32), part, part, part,
                pltpu.SemaphoreType.DMA((3,)),
            ],
            compiler_params=params(4),
            name="pack",
        )(pos[None], pair_count[None], pair_list.T, own, bur, lin)
    with jax.named_scope("weights"):
        weights = pl.pallas_call(
            functools.partial(weight_kernel, blocks),
            out_shape=jax.ShapeDtypeStruct((blocks, 48, FORMS * LANES), jnp.bfloat16),
            in_specs=[VMEM],
            out_specs=VMEM,
            compiler_params=params(8),
            cost_estimate=cost(COST[3]),
            name="weight",
        )(cell)
    sums = jax.ShapeDtypeStruct((7 * blocks, 8, LANES), jnp.float32)

    def near(stage, sources, *others):
        total_cells = sum(s.shape[0] for s in sources)
        jobs = blocks + 2 * rows + total_cells * rows
        extra = [pltpu.VMEM(sums.shape, sums.dtype)] if stage == 2 else []
        with jax.named_scope("near%d" % stage):
            return pl.pallas_call(
                functools.partial(near_kernel, stage, slots, blocks, rows),
                out_shape=jax.ShapeDtypeStruct(own.shape, jnp.float32) if stage == 2 else sums,
                in_specs=[SMEM, SMEM] + [VMEM] * (1 + len(sources) + len(others)),
                out_specs=VMEM,
                scratch_shapes=extra
                + [
                    pltpu.SMEM((jobs,), jnp.int32),
                    pltpu.VMEM((-(-total_cells // 8) * 8, LANES), jnp.int32),
                    pltpu.SMEM((-(-total_cells // 8) * 8, LANES), jnp.int32),
                    pltpu.SemaphoreType.DMA,
                    pltpu.VMEM((LANES, 48), jnp.bfloat16),
                    pltpu.VMEM((LANES, 48), jnp.bfloat16),
                    pltpu.VMEM((LANES, FORMS * LANES), jnp.float32),
                    pltpu.VMEM((LANES, FORMS * LANES), jnp.float32),
                ],
                compiler_params=params(8),
                cost_estimate=cost(COST[stage]),
                name="near%d" % stage,
            )(pos, line, weights, *sources, *others)

    at = 6 * blocks + 1
    level = cell[None]
    moments = level[:, at, :]
    near0 = near(0, [level])
    for axis in ("gy", "gz"):
        carried = moments.shape[0] == level.shape[0]
        with jax.named_scope("halo_" + axis):
            found = neighbours(level, axis)
        step = 1
        if carried and found:
            moments = joined(moments, found[0][:, at, :])
            step = 2
        while step < lax.axis_size(axis):
            moments = joined(moments, crossed(moments, axis, step))
            step *= 2
        level = jnp.concatenate([level] + found, axis=0)
    with jax.named_scope("halo_gx"):
        sides = neighbours(level, "gx")
    near1 = near(1, [level], near0)
    parts = [moments]
    step = 1
    while step < sizes[0]:
        got = crossed(moments, "gx", step)
        parts.append(got)
        step *= 2
        if step < sizes[0]:
            moments = joined(moments, got)
    every = coupling_rows(*sizes)
    with jax.named_scope("couple"):
        table = pl.pallas_call(
            functools.partial(couple_kernel, sizes),
            out_shape=jax.ShapeDtypeStruct((math.prod(sizes), every.shape[1]), jnp.float32),
            in_specs=[SMEM, VMEM],
            out_specs=VMEM,
            compiler_params=params(16),
            cost_estimate=cost(COST[3]),
            name="couple",
        )(pos, jnp.asarray(every))
    with jax.named_scope("local"):
        local = pl.pallas_call(
            local_kernel,
            out_shape=jax.ShapeDtypeStruct((8, LANES), jnp.float32),
            in_specs=[VMEM] * (1 + len(parts)),
            out_specs=VMEM,
            compiler_params=params(16),
            cost_estimate=cost(COST[3]),
            name="local",
        )(table, *parts)
    forces = near(2, sides, near1, cell, local)
    return jnp.swapaxes(forces, 0, 1)[None, None, None]


def solution(mesh):
    return jax.shard_map(
        per_device,
        mesh=mesh,
        in_specs=(
            P("gx", "gy", "gz", None, None, None),
            P("gx", "gy", "gz", None, None, None),
            P("gx", "gy", "gz", None, None, None),
            P(("gx", "gy", "gz"), None),
            P(("gx", "gy", "gz")),
        ),
        out_specs=P("gx", "gy", "gz", None, None, None),
        check_vma=False,
    )
```

```python
import functools
import math

import jax
import jax.numpy as jnp
import numpy as np
from jax import lax
from jax.experimental import pallas as pl
from jax.experimental.pallas import tpu as pltpu
from jax.sharding import PartitionSpec as P

CORE_SQ = 0.0625
AXES = ("gx", "gy", "gz")
LANES = 128
COST = (int(1e9), int(1e9), int(3e9), int(5e8))
LOW = 20
STEP = 24
HIGH = lax.Precision.HIGHEST


def multi_indices(top):
    result = []
    for order in range(top + 1):
        for i in range(order, -1, -1):
            for j in range(order - i, -1, -1):
                result.append((i, j, order - i - j))
    return result


def potential_derivatives(points, top):
    rho = np.sum(points * points, axis=1) + CORE_SQ
    known = {}
    factor = 1.0
    for n in range(top + 1):
        known[(n, 0, 0, 0)] = factor * rho ** (-(n + 0.5))
        factor *= -(2 * n + 1)

    def value(n, index):
        key = (n,) + index
        if key not in known:
            r = [s for s in range(3) if index[s] > 0][0]
            less = list(index)
            less[r] -= 1
            total = points[:, r] * value(n + 1, tuple(less))
            if less[r] > 0:
                lower = list(less)
                lower[r] -= 1
                total = total + less[r] * value(n + 1, tuple(lower))
            known[key] = total
        return known[key]

    return {index: value(0, index) for index in multi_indices(top)}


@functools.lru_cache(maxsize=None)
def coupling_rows(nx, ny, nz):
    grid = np.meshgrid(
        np.arange(-(nx - 1), nx), np.arange(-(ny - 1), ny), np.arange(-(nz - 1), nz), indexing="ij"
    )
    shift = np.stack([g.reshape(-1) for g in grid], axis=1).astype(np.float64)
    table = potential_derivatives(-shift, 6)
    far = (np.max(np.abs(shift), axis=1) > 1.5).astype(np.float64)
    low = multi_indices(3)
    width = -(-LOW * LOW // LANES) * LANES
    rows = np.zeros((shift.shape[0], width), np.float32)
    for a, alpha in enumerate(low):
        for b, beta in enumerate(low):
            index = tuple(alpha[r] + beta[r] for r in range(3))
            rows[:, a * LOW + b] = (-1.0) ** sum(alpha) * table[index] * far
    return rows


def split_const(value, size):
    if size & (size - 1) == 0:
        bits = size.bit_length() - 1
        return jnp.right_shift(value, bits), jnp.bitwise_and(value, size - 1)
    high = lax.div(value, jnp.int32(size))
    return high, value - high * size


def ninths(k):
    nine = jnp.right_shift(k * 57, 9)
    rest = k - 9 * nine
    three = jnp.right_shift(rest * 11, 5)
    return nine - 1, three - 1, rest - 3 * three - 1, rest


def monomial_rows(e):
    rows = []
    for i, j, k in multi_indices(3):
        scale = 1.0 / (math.factorial(i) * math.factorial(j) * math.factorial(k))
        term = None
        for r, power in enumerate((i, j, k)):
            for _ in range(power):
                term = e[r] if term is None else term * e[r]
        if term is None:
            rows.append((None, scale))
        else:
            rows.append((term, scale))
    return rows


def pack_kernel(sizes, slots, blocks, pos_ref, count_ref, pairs_any, off_any, bur_any, lin_any,
                cell_ref, list_ref, part_ref, pairs_ref, off_ref, bur_ref, lin_ref, sems):
    copies = [
        pltpu.make_async_copy(source, target, sems.at[n])
        for n, (source, target) in enumerate(
            (
                (pairs_any, pairs_ref), (off_any, off_ref), (bur_any, bur_ref), (lin_any, lin_ref),
            )
        )
    ]
    for copy in copies:
        copy.start()
    part_ref[...] = jnp.zeros_like(part_ref)
    copies[0].wait()
    rows = pairs_ref.shape[1]
    n = pairs_ref[1:2, :].astype(jnp.float32)
    a = pairs_ref[0:1, :].astype(jnp.float32)
    k = jnp.floor((n + 0.5) * (1.0 / blocks))
    nine = jnp.floor((k + 0.5) * (1.0 / 9.0))
    rest = k - 9.0 * nine
    three = jnp.floor((rest + 0.5) * (1.0 / 3.0))
    one = rest - 3.0 * three
    live = lax.broadcasted_iota(jnp.int32, (1, rows), 1) < count_ref[...]
    for digit, axis in ((nine, 0), (three, 1), (one, 2)):
        where = digit + (pos_ref[:, axis : axis + 1] - 1).astype(jnp.float32)
        live = live & (where >= 0.0) & (where < float(sizes[axis]))
    middle = jnp.where(rest == 4.0, 0.0, jnp.where(rest < 4.0, rest + 1.0, rest))
    spot = jnp.where(nine == 1.0, middle, jnp.where(nine == 0.0, 9.0 + rest, 18.0 + rest))
    spot = jnp.where(live, spot, 27.0)
    code = n * float(blocks) + a
    cell = jnp.zeros_like(n)
    for digit, axis, weight in ((one, 2, slots[1]), (three, 1, 1), (nine, 0, slots[1] * slots[2])):
        first = (1 - 2 * jnp.bitwise_and(pos_ref[:, axis : axis + 1], 1)).astype(jnp.float32)
        slot = jnp.where(digit == 1.0, 0.0, jnp.where(digit - 1.0 == first, 1.0, 2.0))
        cell = cell + float(weight) * (jnp.maximum(slot - 1.0, 0.0) if axis == 0 else slot)
    job = ((cell * 32.0 + k) * float(blocks) + n - float(blocks) * k) * float(blocks) + a
    lane = lax.broadcasted_iota(jnp.int32, (rows, rows), 1)
    down = lax.broadcasted_iota(jnp.int32, (rows, rows), 0)
    spot_c = jnp.sum(jnp.where(lane == down, spot, 0.0), axis=1, keepdims=True)
    code_c = jnp.sum(jnp.where(lane == down, code, 0.0), axis=1, keepdims=True)
    job_c = jnp.sum(jnp.where(lane == down, job, 0.0), axis=1, keepdims=True)
    ahead = (spot < spot_c) | ((spot == spot_c) & (lane < down))
    rank = jnp.sum(jnp.where(ahead, 1.0, 0.0), axis=1, keepdims=True)
    lane_f = lax.broadcasted_iota(jnp.int32, (rows, LANES), 1).astype(jnp.float32)
    ordered = jnp.sum(jnp.where(rank == lane_f, code_c, 0.0), axis=0, keepdims=True)
    jobs = jnp.sum(jnp.where(rank == lane_f, job_c, 0.0), axis=0, keepdims=True)
    starts = jnp.sum(jnp.where(spot_c < lane_f - float(rows), 1.0, 0.0), axis=0, keepdims=True)
    line = jnp.where(lane_f[:1] < float(rows), ordered, starts)
    cell_ref[6 * blocks : 6 * blocks + 8, :] = jnp.broadcast_to(line, (8, LANES))
    line = jnp.where(lane_f[:1] < float(rows), jobs, starts)
    list_ref[...] = jnp.broadcast_to(line, (8, LANES)).astype(jnp.int32)
    for copy in copies[1:]:
        copy.wait()
    e = [off_ref[r] - 0.5 for r in range(3)]
    b = [bur_ref[r] for r in range(3)]
    l = [lin_ref[r] for r in range(3)]
    q = [b[1] * l[2] - b[2] * l[1], b[2] * l[0] - b[0] * l[2], b[0] * l[1] - b[1] * l[0]]
    for r in range(3):
        cell_ref[r * blocks : (r + 1) * blocks, :] = e[r]
        cell_ref[(3 + r) * blocks : (4 + r) * blocks, :] = q[r]
    for m, (term, scale) in enumerate(monomial_rows(e)):
        for r in range(3):
            value = q[r] if term is None else term * q[r]
            line = jnp.sum(value, axis=0, keepdims=True)
            part_ref[r * STEP + m : r * STEP + m + 1, :] = line if scale == 1.0 else line * scale
    turned = part_ref[...].T
    cell_ref[6 * blocks + 1 : 6 * blocks + 2, :] = jnp.sum(turned, axis=0, keepdims=True)


def couple_kernel(sizes, pos_ref, all_ref, out_ref):
    def one(s, carry):
        sx, rest = split_const(s, sizes[1] * sizes[2])
        sz, sy = split_const(rest, sizes[1])
        at = jnp.int32(0)
        for axis, slot in ((0, sx), (1, sy), (2, sz)):
            there = jnp.bitwise_xor(pos_ref[axis], slot)
            at = at * (2 * sizes[axis] - 1) + there - pos_ref[axis] + sizes[axis] - 1
        out_ref[pl.ds(s, 1), :] = all_ref[pl.ds(at, 1), :]
        return carry

    total = out_ref.shape[0]
    trip = math.gcd(total, 8)

    def several(t, carry):
        for n in range(trip):
            one(t * trip + n, carry)
        return carry

    lax.fori_loop(0, total // trip, several, 0)


def thirds(value):
    first = value.astype(jnp.bfloat16).astype(jnp.float32)
    left = value - first
    second = left.astype(jnp.bfloat16).astype(jnp.float32)
    return first, second, left - second


def weight_kernel(blocks, own_ref, out_ref):
    row = lax.broadcasted_iota(jnp.int32, (8, LANES), 0)

    def one(x, carry):
        own = [
            jnp.broadcast_to(own_ref[pl.ds(c * blocks + x, 1), :], (8, LANES)) for c in range(6)
        ]
        m, q = own[:3], own[3:]
        zero = jnp.zeros((8, LANES), jnp.float32)

        def form(entries):
            total = zero
            for at, value in entries:
                total = jnp.where(row == at, value, total)
            return total

        q3 = [3.0 * c for c in q]
        product = q3[0] * m[0] + q3[1] * m[1] + q3[2] * m[2]
        forms = [form([(r, -1.0), (7, m[r])]) for r in range(3)]
        forms.append(form([(3 + r, q[r]) for r in range(3)]))
        forms.append(form([(r, -q3[r]) for r in range(3)] + [(7, product)]))
        forms.append(form([(3 + r, m[r]) for r in range(3)] + [(6, -1.0)]))
        forms += [form([(3 + r, 1.0)]) for r in range(3)]
        for o, value in enumerate(forms):
            p = thirds(value)
            stacked = jnp.concatenate([p[0], p[1], p[2], p[0], p[1], p[0]], axis=0)
            out_ref[x, :, o * LANES : (o + 1) * LANES] = stacked.astype(jnp.bfloat16)
        return carry

    lax.fori_loop(0, blocks, one, 0)


FORMS = 9
WAYS = 4
CHUNK = 128


def near_sum(blocks, weight_ref, sources, job_ref, job_count, acc_ref, scratch):
    left = scratch
    cells_of = sources[0].shape[0]
    row6 = lax.broadcasted_iota(jnp.int32, (6, LANES), 0)

    def unpack(j):
        high, x = split_const(job_ref[j], blocks)
        high, b = split_const(high, blocks)
        cell, k = split_const(high, 32)
        return x, b, cell, k

    def turn(j, slot):
        x, b, cell, k = unpack(j)
        dx, dy, dz, _ = ninths(k)
        if len(sources) == 1:
            y = sources[0][cell, pl.ds(b, 6, stride=blocks), :]
        else:
            local = jnp.where(cell >= cells_of, cell - cells_of, cell)
            y0 = sources[0][local, pl.ds(b, 6, stride=blocks), :]
            y1 = sources[1][local, pl.ds(b, 6, stride=blocks), :]
            y = jnp.where(cell >= cells_of, y1, y0)
        shift = jnp.where(
            row6 == 0, dx, jnp.where(row6 == 1, dy, jnp.where(row6 == 2, dz, 0))
        ).astype(jnp.float32)
        y = y + shift
        product = jnp.sum(y[0:3] * y[3:6], axis=0, keepdims=True)
        y = jnp.concatenate([y, product, jnp.ones((1, LANES), jnp.float32)], axis=0)
        p = thirds(y)
        stacked = jnp.concatenate([p[0], p[0], p[0], p[1], p[1], p[2]], axis=0)
        left[slot][...] = stacked.T.astype(jnp.bfloat16)

    def work(j, slot):
        x = unpack(j)[0]
        total = None
        factors = weight_ref[x]
        for first in range(0, LANES, CHUNK):
            forms = jnp.dot(
                left[slot][first : first + CHUNK, :], factors, preferred_element_type=jnp.float32
            )
            for t in range(CHUNK // 8):
                f = [
                    forms[8 * t : 8 * t + 8, o * LANES : (o + 1) * LANES] for o in range(FORMS)
                ]
                r, alike, u3, v, q = f[:3], f[3], f[4], f[5], f[6:]
                square = (r[0] * r[0] + r[1] * r[1]) + (r[2] * r[2] + CORE_SQ)
                s = lax.rsqrt(square)
                s2 = s * s
                s3 = s2 * s
                w = s3 * (alike + (u3 * v) * s2)
                u3s = u3 * s3
                terms = [w * r[0], w * r[1], w * r[2]]
                terms += [u3s * q[0], u3s * q[1], u3s * q[2], v * s3]
                total = terms if total is None else [p + n for p, n in zip(total, terms)]
        for c in range(7):
            acc_ref[7 * x + c] += total[c]

    @pl.when(job_count > 0)
    def _():
        last = job_count - 1
        for slot in range(WAYS):
            turn(jnp.minimum(slot, last), slot)

        def several(i, carry):
            for slot in range(WAYS):
                j = WAYS * i + slot
                work(j, slot)
                turn(jnp.minimum(j + WAYS, last), slot)
            return carry

        whole = job_count // WAYS
        lax.fori_loop(0, whole, several, 0)
        for slot in range(WAYS - 1):

            @pl.when(whole * WAYS + slot < job_count)
            def _():
                work(whole * WAYS + slot, slot)


def put_jobs(job_ref, count, list_ref, row, begin, end):
    def one(r, count):
        job_ref[count] = list_ref[row, r]
        return count + 1

    return lax.fori_loop(begin, end, one, count)


def near_forces(blocks, own_ref, acc_ref):
    out = [[], [], []]
    for x in range(blocks):
        sums = [jnp.sum(acc_ref[7 * x + c], axis=0, keepdims=True) for c in range(7)]
        for r in range(3):
            q = own_ref[(3 + r) * blocks + x : (3 + r) * blocks + x + 1, :]
            out[r].append(sums[r] - sums[3 + r] * (1.0 / 3.0) - q * sums[6])
    return [jnp.concatenate(o, axis=0) for o in out]


def slot_delta(slot, place):
    if slot == 0:
        return jnp.int32(0)
    first = 1 - 2 * jnp.bitwise_and(place, 1)
    return first if slot == 1 else -first


def near_kernel(stage, slots, blocks, rows, pos_ref, list_ref, weight_ref, *refs):
    scratch = refs[-WAYS:]
    refs = refs[:-WAYS]
    job_ref, ints_ref, lists_ref, sem = refs[-4:]
    if stage == 0:
        own_ref, acc_ref = refs[:2]
        sources = [own_ref]
        acc_ref[...] = jnp.zeros_like(acc_ref)
    elif stage == 1:
        sources = [refs[0]]
        before_ref, acc_ref = refs[1:3]
    else:
        sources = refs[:-9]
        before_ref, own_ref, local_ref, out_ref, acc_ref = refs[-9:-4]
    per = slots[1] * slots[2]
    begin = {0: 0, 1: 1, 2: 9}[stage]
    end = {0: 1, 1: 9, 2: 27}[stage]
    bits = blocks.bit_length() - 1
    lane = lax.broadcasted_iota(jnp.int32, (1, LANES), 1)
    wide = [jnp.broadcast_to(pos_ref[:, r : r + 1], (1, LANES)) for r in range(3)]
    theirs = []
    for side, source in enumerate(sources):
        for cell in range(source.shape[0]):
            if stage == 1 and cell == 0:
                continue
            row = len(theirs)
            dx = slot_delta(side + 1 if stage == 2 else 0, wide[0])
            dy = slot_delta(cell % slots[1], wide[1])
            dz = slot_delta(cell // slots[1], wide[2])
            k = 9 * (dx + 1) + 3 * (dy + 1) + dz + 1
            code = source[cell, 6 * blocks : 6 * blocks + 1, :].astype(jnp.int32)
            a = jnp.bitwise_and(code, blocks - 1)
            b = jnp.bitwise_and(jnp.right_shift(code, bits), blocks - 1)
            turned = jnp.left_shift(a, bits) + b + ((side * per + cell) * 32 + k) * (blocks * blocks)
            ints_ref[row : row + 1, :] = jnp.where(lane < rows, turned, code)
            theirs.append((row, side, cell))
    own_row = len(theirs)
    ints_ref[own_row : own_row + 1, :] = list_ref[0:1, :]
    place = jnp.where(lane == 0, wide[0], jnp.where(lane == 1, wide[1], wide[2]))
    ints_ref[own_row + 1 : own_row + 2, :] = place
    copy = pltpu.make_async_copy(ints_ref, lists_ref, sem)
    copy.start()
    if stage > 0:
        acc_ref[...] = before_ref[...]
    count = jnp.int32(0)
    if stage == 0:
        def self_job(x, count):
            job_ref[count] = (13 * blocks + x) * blocks + x
            return count + 1

        count = lax.fori_loop(0, blocks, self_job, count)
    copy.wait()
    count = put_jobs(
        job_ref, count, lists_ref, own_row,
        lists_ref[own_row, rows + begin], lists_ref[own_row, rows + end],
    )
    for row, side, cell in theirs:
        dx = slot_delta(side + 1 if stage == 2 else 0, lists_ref[own_row + 1, 0])
        dy = slot_delta(cell % slots[1], lists_ref[own_row + 1, 1])
        dz = slot_delta(cell // slots[1], lists_ref[own_row + 1, 2])
        rest = 3 * (1 - dy) + 1 - dz
        if stage == 0:
            spot = jnp.int32(0)
        elif stage == 1:
            spot = jnp.where(rest < 4, rest + 1, rest)
        else:
            spot = jnp.where(dx < 0, 18, 9) + rest
        count = put_jobs(
            job_ref, count, lists_ref, row,
            lists_ref[row, rows + spot], lists_ref[row, rows + spot + 1],
        )
    near_sum(blocks, weight_ref, sources, job_ref, count, acc_ref, scratch)
    if stage == 2:
        near = near_forces(blocks, own_ref, acc_ref)
        far = far_forces(blocks, own_ref, local_ref[...])
        for r in range(3):
            out_ref[r] = near[r] + far[r]


@functools.lru_cache(maxsize=None)
def sum_masks(width):
    row = np.arange(3 * STEP)[:, None] % STEP
    col = np.arange(width)
    keep = (row == col[None] // LOW) & (col[None] < LOW * LOW)
    fold = (col[:, None] % LOW == np.arange(LANES)[None]) & (col[:, None] < LOW * LOW)
    return keep.astype(np.float32), fold.astype(np.float32)


def local_kernel(table_ref, keep_ref, fold_ref, *refs):
    parts, out_ref = refs[:-1], refs[-1]
    moments = jnp.concatenate([part[...] for part in parts], axis=0)
    every = lax.dot_general(
        moments, table_ref[...], (((0,), (0,)), ((), ())),
        precision=HIGH, preferred_element_type=jnp.float32,
    )
    every = every[: 3 * STEP] * keep_ref[...]
    sums = [jnp.sum(every[STEP * r : STEP * (r + 1)], axis=0, keepdims=True) for r in range(3)]
    sums = jnp.concatenate(sums + [jnp.zeros((5, every.shape[1]), jnp.float32)], axis=0)
    stacked = jnp.concatenate(list(thirds(sums)), axis=0).astype(jnp.bfloat16)
    local = jnp.dot(stacked, fold_ref[...], preferred_element_type=jnp.float32)
    out_ref[...] = local[0:8] + local[8:16] + local[16:24]


def far_forces(blocks, own_ref, local):
    e = [own_ref[r * blocks : (r + 1) * blocks, :] for r in range(3)]
    q = [own_ref[(3 + r) * blocks : (4 + r) * blocks, :] for r in range(3)]
    low = multi_indices(3)
    where_low = {m: n for n, m in enumerate(low)}
    projected = [
        sum(q[d] * jnp.broadcast_to(local[d : d + 1, m : m + 1], q[d].shape) for d in range(3))
        for m in range(LOW)
    ]
    out = []
    for r in range(3):
        far = None
        for g, (term, scale) in zip(low[:10], monomial_rows(e)[:10]):
            up = tuple(g[s] + (1 if s == r else 0) for s in range(3))
            value = projected[where_low[up]]
            if scale != 1.0:
                value = value * scale
            if term is not None:
                value = value * term
            far = value if far is None else far + value
        out.append(-far)
    return out


def joined(first, second):
    rest = [(0, 0)] * (first.ndim - 1)
    above = jnp.pad(first, [(0, second.shape[0])] + rest)
    return above + jnp.pad(second, [(first.shape[0], 0)] + rest)


def neighbours(value, axis):
    count = lax.axis_size(axis)
    found = []
    for first in range(min(count - 1, 2)):
        route = []
        for i in range(first, count - 1, 2):
            route += [(i, i + 1), (i + 1, i)]
        found.append(lax.ppermute(value, axis, route))
    return found


def crossed(value, axis, step):
    return lax.ppermute(value, axis, [(i, i ^ step) for i in range(lax.axis_size(axis))])


HBM = pl.BlockSpec(memory_space=pltpu.HBM)
VMEM = pl.BlockSpec(memory_space=pltpu.VMEM)
SMEM = pl.BlockSpec(memory_space=pltpu.SMEM)


def cost(flops):
    return pl.CostEstimate(flops=flops, bytes_accessed=1 << 20, transcendentals=0)


def params(mib):
    return pltpu.CompilerParams(vmem_limit_bytes=mib * 1024 * 1024)


def per_device(offsets, burgers, lines, pair_list, pair_count):
    blocks = offsets.shape[3]
    width = offsets.shape[5]
    sizes = tuple(lax.axis_size(a) for a in AXES)
    place = [lax.axis_index(a).astype(jnp.int32) for a in AXES]
    pos = jnp.stack(place)
    rows = pair_list.shape[0]
    for size in sizes:
        assert size & (size - 1) == 0
    own, bur, lin = (jnp.swapaxes(v[0, 0, 0], 0, 1) for v in (offsets, burgers, lines))
    cell_rows = 6 * blocks + 8
    slots = tuple(min(s, 3) for s in sizes)
    part = pltpu.VMEM(own.shape, jnp.float32)
    with jax.named_scope("packing"):
        cell, line = pl.pallas_call(
            functools.partial(pack_kernel, sizes, slots, blocks),
            out_shape=(
                jax.ShapeDtypeStruct((cell_rows, width), jnp.float32),
                jax.ShapeDtypeStruct((8, width), jnp.int32),
            ),
            in_specs=[VMEM] * 2 + [HBM] * 4,
            out_specs=(VMEM, VMEM),
            scratch_shapes=[
                pltpu.VMEM((LANES, LANES), jnp.float32),
                pltpu.VMEM((2, rows), jnp.int32), part, part, part,
                pltpu.SemaphoreType.DMA((4,)),
            ],
            compiler_params=params(4),
            name="pack",
        )(
            pos[None],
            pair_count[None],
            *[
                pltpu.with_memory_space_constraint(v, pltpu.HBM)
                for v in (pair_list.T, own, bur, lin)
            ],
        )
    with jax.named_scope("weights"):
        weights = pl.pallas_call(
            functools.partial(weight_kernel, blocks),
            out_shape=jax.ShapeDtypeStruct((blocks, 48, FORMS * LANES), jnp.bfloat16),
            in_specs=[VMEM],
            out_specs=VMEM,
            compiler_params=params(8),
            cost_estimate=cost(COST[3]),
            name="weight",
        )(cell)
    sums = jax.ShapeDtypeStruct((7 * blocks, 8, LANES), jnp.float32)

    def near(stage, sources, *others):
        total_cells = sum(s.shape[0] for s in sources)
        jobs = blocks + 2 * rows + total_cells * rows
        extra = [pltpu.VMEM(sums.shape, sums.dtype)] if stage == 2 else []
        with jax.named_scope("near%d" % stage):
            return pl.pallas_call(
                functools.partial(near_kernel, stage, slots, blocks, rows),
                out_shape=jax.ShapeDtypeStruct(own.shape, jnp.float32) if stage == 2 else sums,
                in_specs=[VMEM] * (3 + len(sources) + len(others)),
                out_specs=VMEM,
                scratch_shapes=extra
                + [
                    pltpu.SMEM((jobs,), jnp.int32),
                    pltpu.VMEM((-(-(total_cells + 2) // 8) * 8, LANES), jnp.int32),
                    pltpu.SMEM((-(-(total_cells + 2) // 8) * 8, LANES), jnp.int32),
                    pltpu.SemaphoreType.DMA,
                ]
                + [pltpu.VMEM((LANES, 48), jnp.bfloat16)] * WAYS,
                compiler_params=params(8),
                cost_estimate=cost(COST[stage]),
                name="near%d" % stage,
            )(pos[None], line, weights, *sources, *others)

    every = coupling_rows(*sizes)
    with jax.named_scope("couple"):
        table = pl.pallas_call(
            functools.partial(couple_kernel, sizes),
            out_shape=jax.ShapeDtypeStruct((math.prod(sizes), every.shape[1]), jnp.float32),
            in_specs=[SMEM, VMEM],
            out_specs=VMEM,
            compiler_params=params(16),
            cost_estimate=cost(COST[3]),
            name="couple",
        )(pos, jnp.asarray(every))
    at = 6 * blocks + 1
    level = cell[None]
    moments = level[:, at, :]
    near0 = near(0, [level])
    for axis in ("gy", "gz"):
        carried = moments.shape[0] == level.shape[0]
        with jax.named_scope("halo_" + axis):
            found = neighbours(level, axis)
        if axis == "gz" and found:
            found[-1], table = lax.optimization_barrier((found[-1], table))
        step = 1
        if carried and found:
            moments = joined(moments, found[0][:, at, :])
            step = 2
        while step < lax.axis_size(axis):
            moments = joined(moments, crossed(moments, axis, step))
            step *= 2
        level = jnp.concatenate([level] + found, axis=0)
    with jax.named_scope("halo_gx"):
        sides = neighbours(level, "gx")
    near1 = near(1, [level], near0)
    parts = [moments]
    step = 1
    while step < sizes[0]:
        got = crossed(moments, "gx", step)
        parts.append(got)
        step *= 2
        if step < sizes[0]:
            moments = joined(moments, got)
    keep, fold = sum_masks(every.shape[1])
    with jax.named_scope("local"):
        local = pl.pallas_call(
            local_kernel,
            out_shape=jax.ShapeDtypeStruct((8, LANES), jnp.float32),
            in_specs=[VMEM] * (3 + len(parts)),
            out_specs=VMEM,
            compiler_params=params(16),
            cost_estimate=cost(COST[3]),
            name="local",
        )(table, jnp.asarray(keep), jnp.asarray(fold, jnp.bfloat16), *parts)
    forces = near(2, sides, near1, cell, local)
    return jnp.swapaxes(forces, 0, 1)[None, None, None]


def solution(mesh):
    return jax.shard_map(
        per_device,
        mesh=mesh,
        in_specs=(
            P("gx", "gy", "gz", None, None, None),
            P("gx", "gy", "gz", None, None, None),
            P("gx", "gy", "gz", None, None, None),
            P(("gx", "gy", "gz"), None),
            P(("gx", "gy", "gz")),
        ),
        out_specs=P("gx", "gy", "gz", None, None, None),
        check_vma=False,
    )
```

```python
import functools
import math

import jax
import jax.numpy as jnp
import numpy as np
from jax import lax
from jax.experimental import pallas as pl
from jax.experimental.pallas import tpu as pltpu
from jax.sharding import PartitionSpec as P

CORE_SQ = 0.0625
AXES = ("gx", "gy", "gz")
LANES = 128
COST = (int(1e9), int(1e9), int(3e9), int(5e8))
LOW = 20
STEP = 24
HIGH = lax.Precision.HIGHEST


def multi_indices(top):
    result = []
    for order in range(top + 1):
        for i in range(order, -1, -1):
            for j in range(order - i, -1, -1):
                result.append((i, j, order - i - j))
    return result


def potential_derivatives(points, top):
    rho = np.sum(points * points, axis=1) + CORE_SQ
    known = {}
    factor = 1.0
    for n in range(top + 1):
        known[(n, 0, 0, 0)] = factor * rho ** (-(n + 0.5))
        factor *= -(2 * n + 1)

    def value(n, index):
        key = (n,) + index
        if key not in known:
            r = [s for s in range(3) if index[s] > 0][0]
            less = list(index)
            less[r] -= 1
            total = points[:, r] * value(n + 1, tuple(less))
            if less[r] > 0:
                lower = list(less)
                lower[r] -= 1
                total = total + less[r] * value(n + 1, tuple(lower))
            known[key] = total
        return known[key]

    return {index: value(0, index) for index in multi_indices(top)}


@functools.lru_cache(maxsize=None)
def coupling_rows(nx, ny, nz):
    grid = np.meshgrid(
        np.arange(-(nx - 1), nx), np.arange(-(ny - 1), ny), np.arange(-(nz - 1), nz), indexing="ij"
    )
    shift = np.stack([g.reshape(-1) for g in grid], axis=1).astype(np.float64)
    table = potential_derivatives(-shift, 6)
    far = (np.max(np.abs(shift), axis=1) > 1.5).astype(np.float64)
    low = multi_indices(3)
    width = -(-LOW * LOW // LANES) * LANES
    rows = np.zeros((shift.shape[0], width), np.float32)
    for a, alpha in enumerate(low):
        for b, beta in enumerate(low):
            index = tuple(alpha[r] + beta[r] for r in range(3))
            rows[:, a * LOW + b] = (-1.0) ** sum(alpha) * table[index] * far
    return rows


def split_const(value, size):
    if size & (size - 1) == 0:
        bits = size.bit_length() - 1
        return jnp.right_shift(value, bits), jnp.bitwise_and(value, size - 1)
    high = lax.div(value, jnp.int32(size))
    return high, value - high * size


def ninths(k):
    nine = jnp.right_shift(k * 57, 9)
    rest = k - 9 * nine
    three = jnp.right_shift(rest * 11, 5)
    return nine - 1, three - 1, rest - 3 * three - 1, rest


def monomial_rows(e):
    rows = []
    for i, j, k in multi_indices(3):
        scale = 1.0 / (math.factorial(i) * math.factorial(j) * math.factorial(k))
        term = None
        for r, power in enumerate((i, j, k)):
            for _ in range(power):
                term = e[r] if term is None else term * e[r]
        if term is None:
            rows.append((None, scale))
        else:
            rows.append((term, scale))
    return rows


def pack_kernel(sizes, slots, blocks, pos_ref, count_ref, pairs_any, off_any, bur_any, lin_any,
                cell_ref, list_ref, part_ref, pairs_ref, off_ref, bur_ref, lin_ref, sems):
    copies = [
        pltpu.make_async_copy(source, target, sems.at[n])
        for n, (source, target) in enumerate(
            (
                (pairs_any, pairs_ref), (off_any, off_ref), (bur_any, bur_ref), (lin_any, lin_ref),
            )
        )
    ]
    for copy in copies:
        copy.start()
    part_ref[...] = jnp.zeros_like(part_ref)
    copies[0].wait()
    rows = pairs_ref.shape[1]
    n = pairs_ref[1:2, :].astype(jnp.float32)
    a = pairs_ref[0:1, :].astype(jnp.float32)
    k = jnp.floor((n + 0.5) * (1.0 / blocks))
    nine = jnp.floor((k + 0.5) * (1.0 / 9.0))
    rest = k - 9.0 * nine
    three = jnp.floor((rest + 0.5) * (1.0 / 3.0))
    one = rest - 3.0 * three
    live = lax.broadcasted_iota(jnp.int32, (1, rows), 1) < count_ref[...]
    for digit, axis in ((nine, 0), (three, 1), (one, 2)):
        where = digit + (pos_ref[:, axis : axis + 1] - 1).astype(jnp.float32)
        live = live & (where >= 0.0) & (where < float(sizes[axis]))
    middle = jnp.where(rest == 4.0, 0.0, jnp.where(rest < 4.0, rest + 1.0, rest))
    spot = jnp.where(nine == 1.0, middle, jnp.where(nine == 0.0, 9.0 + rest, 18.0 + rest))
    spot = jnp.where(live, spot, 27.0)
    code = n * float(blocks) + a
    cell = jnp.zeros_like(n)
    for digit, axis, weight in ((one, 2, slots[1]), (three, 1, 1), (nine, 0, slots[1] * slots[2])):
        first = (1 - 2 * jnp.bitwise_and(pos_ref[:, axis : axis + 1], 1)).astype(jnp.float32)
        slot = jnp.where(digit == 1.0, 0.0, jnp.where(digit - 1.0 == first, 1.0, 2.0))
        cell = cell + float(weight) * (jnp.maximum(slot - 1.0, 0.0) if axis == 0 else slot)
    job = ((cell * 32.0 + k) * float(blocks) + n - float(blocks) * k) * float(blocks) + a
    lane = lax.broadcasted_iota(jnp.int32, (rows, rows), 1)
    down = lax.broadcasted_iota(jnp.int32, (rows, rows), 0)
    spot_c = jnp.sum(jnp.where(lane == down, spot, 0.0), axis=1, keepdims=True)
    code_c = jnp.sum(jnp.where(lane == down, code, 0.0), axis=1, keepdims=True)
    job_c = jnp.sum(jnp.where(lane == down, job, 0.0), axis=1, keepdims=True)
    ahead = (spot < spot_c) | ((spot == spot_c) & (lane < down))
    rank = jnp.sum(jnp.where(ahead, 1.0, 0.0), axis=1, keepdims=True)
    lane_f = lax.broadcasted_iota(jnp.int32, (rows, LANES), 1).astype(jnp.float32)
    ordered = jnp.sum(jnp.where(rank == lane_f, code_c, 0.0), axis=0, keepdims=True)
    jobs = jnp.sum(jnp.where(rank == lane_f, job_c, 0.0), axis=0, keepdims=True)
    starts = jnp.sum(jnp.where(spot_c < lane_f - float(rows), 1.0, 0.0), axis=0, keepdims=True)
    line = jnp.where(lane_f[:1] < float(rows), ordered, starts)
    cell_ref[6 * blocks : 6 * blocks + 8, :] = jnp.broadcast_to(line, (8, LANES))
    line = jnp.where(lane_f[:1] < float(rows), jobs, starts)
    list_ref[...] = jnp.broadcast_to(line, (8, LANES)).astype(jnp.int32)
    for copy in copies[1:]:
        copy.wait()
    e = [off_ref[r] - 0.5 for r in range(3)]
    b = [bur_ref[r] for r in range(3)]
    l = [lin_ref[r] for r in range(3)]
    q = [b[1] * l[2] - b[2] * l[1], b[2] * l[0] - b[0] * l[2], b[0] * l[1] - b[1] * l[0]]
    for r in range(3):
        cell_ref[r * blocks : (r + 1) * blocks, :] = e[r]
        cell_ref[(3 + r) * blocks : (4 + r) * blocks, :] = q[r]
    for m, (term, scale) in enumerate(monomial_rows(e)):
        for r in range(3):
            value = q[r] if term is None else term * q[r]
            line = jnp.sum(value, axis=0, keepdims=True)
            part_ref[r * STEP + m : r * STEP + m + 1, :] = line if scale == 1.0 else line * scale
    turned = part_ref[...].T
    cell_ref[6 * blocks + 1 : 6 * blocks + 2, :] = jnp.sum(turned, axis=0, keepdims=True)


def couple_kernel(sizes, pos_ref, all_ref, out_ref):
    def one(s, carry):
        sx, rest = split_const(s, sizes[1] * sizes[2])
        sz, sy = split_const(rest, sizes[1])
        at = jnp.int32(0)
        for axis, slot in ((0, sx), (1, sy), (2, sz)):
            there = jnp.bitwise_xor(pos_ref[axis], slot)
            at = at * (2 * sizes[axis] - 1) + there - pos_ref[axis] + sizes[axis] - 1
        out_ref[pl.ds(s, 1), :] = all_ref[pl.ds(at, 1), :]
        return carry

    total = out_ref.shape[0]
    trip = math.gcd(total, 8)

    def several(t, carry):
        for n in range(trip):
            one(t * trip + n, carry)
        return carry

    lax.fori_loop(0, total // trip, several, 0)


def thirds(value):
    first = value.astype(jnp.bfloat16).astype(jnp.float32)
    left = value - first
    second = left.astype(jnp.bfloat16).astype(jnp.float32)
    return first, second, left - second


def weight_kernel(blocks, own_ref, out_ref):
    row = lax.broadcasted_iota(jnp.int32, (8, LANES), 0)

    def one(x, carry):
        own = [
            jnp.broadcast_to(own_ref[pl.ds(c * blocks + x, 1), :], (8, LANES)) for c in range(6)
        ]
        m, q = own[:3], own[3:]
        zero = jnp.zeros((8, LANES), jnp.float32)

        def form(entries):
            total = zero
            for at, value in entries:
                total = jnp.where(row == at, value, total)
            return total

        q3 = [3.0 * c for c in q]
        product = q3[0] * m[0] + q3[1] * m[1] + q3[2] * m[2]
        forms = [form([(r, -1.0), (7, m[r])]) for r in range(3)]
        forms.append(form([(3 + r, q[r]) for r in range(3)]))
        forms.append(form([(r, -q3[r]) for r in range(3)] + [(7, product)]))
        forms.append(form([(3 + r, m[r]) for r in range(3)] + [(6, -1.0)]))
        forms += [form([(3 + r, 1.0)]) for r in range(3)]
        for o, value in enumerate(forms):
            p = thirds(value)
            stacked = jnp.concatenate([p[0], p[1], p[2], p[0], p[1], p[0]], axis=0)
            out_ref[x, :, o * LANES : (o + 1) * LANES] = stacked.astype(jnp.bfloat16)
        return carry

    lax.fori_loop(0, blocks, one, 0)


FORMS = 9
WAYS = 8
CHUNK = 128


def near_sum(blocks, weight_ref, sources, job_ref, job_count, acc_ref, scratch):
    left = scratch
    cells_of = sources[0].shape[0]
    row6 = lax.broadcasted_iota(jnp.int32, (6, LANES), 0)

    def unpack(j):
        high, x = split_const(job_ref[j], blocks)
        high, b = split_const(high, blocks)
        cell, k = split_const(high, 32)
        return x, b, cell, k

    def turn(j, slot):
        x, b, cell, k = unpack(j)
        dx, dy, dz, _ = ninths(k)
        if len(sources) == 1:
            y = sources[0][cell, pl.ds(b, 6, stride=blocks), :]
        else:
            local = jnp.where(cell >= cells_of, cell - cells_of, cell)
            y0 = sources[0][local, pl.ds(b, 6, stride=blocks), :]
            y1 = sources[1][local, pl.ds(b, 6, stride=blocks), :]
            y = jnp.where(cell >= cells_of, y1, y0)
        shift = jnp.where(
            row6 == 0, dx, jnp.where(row6 == 1, dy, jnp.where(row6 == 2, dz, 0))
        ).astype(jnp.float32)
        y = y + shift
        product = jnp.sum(y[0:3] * y[3:6], axis=0, keepdims=True)
        y = jnp.concatenate([y, product, jnp.ones((1, LANES), jnp.float32)], axis=0)
        p = thirds(y)
        stacked = jnp.concatenate([p[0], p[0], p[0], p[1], p[1], p[2]], axis=0)
        left[slot][...] = stacked.T.astype(jnp.bfloat16)

    def work(j, slot):
        x = unpack(j)[0]
        total = None
        factors = weight_ref[x]
        for first in range(0, LANES, CHUNK):
            forms = jnp.dot(
                left[slot][first : first + CHUNK, :], factors, preferred_element_type=jnp.float32
            )
            for t in range(CHUNK // 8):
                f = [
                    forms[8 * t : 8 * t + 8, o * LANES : (o + 1) * LANES] for o in range(FORMS)
                ]
                r, alike, u3, v, q = f[:3], f[3], f[4], f[5], f[6:]
                square = (r[0] * r[0] + r[1] * r[1]) + (r[2] * r[2] + CORE_SQ)
                s = lax.rsqrt(square)
                s2 = s * s
                s3 = s2 * s
                w = s3 * (alike + (u3 * v) * s2)
                u3s = u3 * s3
                terms = [w * r[0], w * r[1], w * r[2]]
                terms += [u3s * q[0], u3s * q[1], u3s * q[2], v * s3]
                total = terms if total is None else [p + n for p, n in zip(total, terms)]
        for c in range(7):
            acc_ref[7 * x + c] += total[c]

    @pl.when(job_count > 0)
    def _():
        last = job_count - 1
        for slot in range(WAYS):
            turn(jnp.minimum(slot, last), slot)

        def several(i, carry):
            for slot in range(WAYS):
                j = WAYS * i + slot
                work(j, slot)
                turn(jnp.minimum(j + WAYS, last), slot)
            return carry

        whole = job_count // WAYS
        lax.fori_loop(0, whole, several, 0)
        for slot in range(WAYS - 1):

            @pl.when(whole * WAYS + slot < job_count)
            def _():
                work(whole * WAYS + slot, slot)


def put_jobs(job_ref, count, list_ref, row, begin, end):
    def one(r, count):
        job_ref[count] = list_ref[row, r]
        return count + 1

    return lax.fori_loop(begin, end, one, count)


def near_forces(blocks, own_ref, acc_ref):
    out = [[], [], []]
    for x in range(blocks):
        sums = [jnp.sum(acc_ref[7 * x + c], axis=0, keepdims=True) for c in range(7)]
        for r in range(3):
            q = own_ref[(3 + r) * blocks + x : (3 + r) * blocks + x + 1, :]
            out[r].append(sums[r] - sums[3 + r] * (1.0 / 3.0) - q * sums[6])
    return [jnp.concatenate(o, axis=0) for o in out]


def slot_delta(slot, place):
    if slot == 0:
        return jnp.int32(0)
    first = 1 - 2 * jnp.bitwise_and(place, 1)
    return first if slot == 1 else -first


def near_kernel(stage, slots, blocks, rows, pos_ref, list_ref, weight_ref, *refs):
    scratch = refs[-WAYS:]
    refs = refs[:-WAYS]
    job_ref, ints_ref, lists_ref, sem = refs[-4:]
    if stage == 0:
        own_ref, acc_ref = refs[:2]
        sources = [own_ref]
        acc_ref[...] = jnp.zeros_like(acc_ref)
    elif stage == 1:
        sources = [refs[0]]
        before_ref, acc_ref = refs[1:3]
    else:
        sources = refs[:-9]
        before_ref, own_ref, local_ref, out_ref, acc_ref = refs[-9:-4]
    per = slots[1] * slots[2]
    begin = {0: 0, 1: 1, 2: 9}[stage]
    end = {0: 1, 1: 9, 2: 27}[stage]
    bits = blocks.bit_length() - 1
    lane = lax.broadcasted_iota(jnp.int32, (1, LANES), 1)
    wide = [jnp.broadcast_to(pos_ref[:, r : r + 1], (1, LANES)) for r in range(3)]
    theirs = []
    for side, source in enumerate(sources):
        for cell in range(source.shape[0]):
            if stage == 1 and cell == 0:
                continue
            row = len(theirs)
            dx = slot_delta(side + 1 if stage == 2 else 0, wide[0])
            dy = slot_delta(cell % slots[1], wide[1])
            dz = slot_delta(cell // slots[1], wide[2])
            k = 9 * (dx + 1) + 3 * (dy + 1) + dz + 1
            code = source[cell, 6 * blocks : 6 * blocks + 1, :].astype(jnp.int32)
            a = jnp.bitwise_and(code, blocks - 1)
            b = jnp.bitwise_and(jnp.right_shift(code, bits), blocks - 1)
            turned = jnp.left_shift(a, bits) + b + ((side * per + cell) * 32 + k) * (blocks * blocks)
            ints_ref[row : row + 1, :] = jnp.where(lane < rows, turned, code)
            theirs.append((row, side, cell))
    own_row = len(theirs)
    ints_ref[own_row : own_row + 1, :] = list_ref[0:1, :]
    place = jnp.where(lane == 0, wide[0], jnp.where(lane == 1, wide[1], wide[2]))
    ints_ref[own_row + 1 : own_row + 2, :] = place
    copy = pltpu.make_async_copy(ints_ref, lists_ref, sem)
    copy.start()
    if stage > 0:
        acc_ref[...] = before_ref[...]
    count = jnp.int32(0)
    if stage == 0:
        def self_job(x, count):
            job_ref[count] = (13 * blocks + x) * blocks + x
            return count + 1

        count = lax.fori_loop(0, blocks, self_job, count)
    copy.wait()
    count = put_jobs(
        job_ref, count, lists_ref, own_row,
        lists_ref[own_row, rows + begin], lists_ref[own_row, rows + end],
    )
    for row, side, cell in theirs:
        dx = slot_delta(side + 1 if stage == 2 else 0, lists_ref[own_row + 1, 0])
        dy = slot_delta(cell % slots[1], lists_ref[own_row + 1, 1])
        dz = slot_delta(cell // slots[1], lists_ref[own_row + 1, 2])
        rest = 3 * (1 - dy) + 1 - dz
        if stage == 0:
            spot = jnp.int32(0)
        elif stage == 1:
            spot = jnp.where(rest < 4, rest + 1, rest)
        else:
            spot = jnp.where(dx < 0, 18, 9) + rest
        count = put_jobs(
            job_ref, count, lists_ref, row,
            lists_ref[row, rows + spot], lists_ref[row, rows + spot + 1],
        )
    near_sum(blocks, weight_ref, sources, job_ref, count, acc_ref, scratch)
    if stage == 2:
        near = near_forces(blocks, own_ref, acc_ref)
        far = far_forces(blocks, own_ref, local_ref[...])
        for r in range(3):
            out_ref[r] = near[r] + far[r]


@functools.lru_cache(maxsize=None)
def sum_masks(width):
    row = np.arange(3 * STEP)[:, None] % STEP
    col = np.arange(width)
    keep = (row == col[None] // LOW) & (col[None] < LOW * LOW)
    fold = (col[:, None] % LOW == np.arange(LANES)[None]) & (col[:, None] < LOW * LOW)
    return keep.astype(np.float32), fold.astype(np.float32)


def local_kernel(table_ref, keep_ref, fold_ref, *refs):
    parts, out_ref = refs[:-1], refs[-1]
    moments = jnp.concatenate([part[...] for part in parts], axis=0)
    every = lax.dot_general(
        moments, table_ref[...], (((0,), (0,)), ((), ())),
        precision=HIGH, preferred_element_type=jnp.float32,
    )
    every = every[: 3 * STEP] * keep_ref[...]
    sums = [jnp.sum(every[STEP * r : STEP * (r + 1)], axis=0, keepdims=True) for r in range(3)]
    sums = jnp.concatenate(sums + [jnp.zeros((5, every.shape[1]), jnp.float32)], axis=0)
    stacked = jnp.concatenate(list(thirds(sums)), axis=0).astype(jnp.bfloat16)
    local = jnp.dot(stacked, fold_ref[...], preferred_element_type=jnp.float32)
    out_ref[...] = local[0:8] + local[8:16] + local[16:24]


def far_forces(blocks, own_ref, local):
    e = [own_ref[r * blocks : (r + 1) * blocks, :] for r in range(3)]
    q = [own_ref[(3 + r) * blocks : (4 + r) * blocks, :] for r in range(3)]
    low = multi_indices(3)
    where_low = {m: n for n, m in enumerate(low)}
    projected = [
        sum(q[d] * jnp.broadcast_to(local[d : d + 1, m : m + 1], q[d].shape) for d in range(3))
        for m in range(LOW)
    ]
    out = []
    for r in range(3):
        far = None
        for g, (term, scale) in zip(low[:10], monomial_rows(e)[:10]):
            up = tuple(g[s] + (1 if s == r else 0) for s in range(3))
            value = projected[where_low[up]]
            if scale != 1.0:
                value = value * scale
            if term is not None:
                value = value * term
            far = value if far is None else far + value
        out.append(-far)
    return out


def joined(first, second):
    rest = [(0, 0)] * (first.ndim - 1)
    above = jnp.pad(first, [(0, second.shape[0])] + rest)
    return above + jnp.pad(second, [(first.shape[0], 0)] + rest)


def neighbours(value, axis):
    count = lax.axis_size(axis)
    found = []
    for first in range(min(count - 1, 2)):
        route = []
        for i in range(first, count - 1, 2):
            route += [(i, i + 1), (i + 1, i)]
        found.append(lax.ppermute(value, axis, route))
    return found


def crossed(value, axis, step):
    return lax.ppermute(value, axis, [(i, i ^ step) for i in range(lax.axis_size(axis))])


HBM = pl.BlockSpec(memory_space=pltpu.HBM)
VMEM = pl.BlockSpec(memory_space=pltpu.VMEM)
SMEM = pl.BlockSpec(memory_space=pltpu.SMEM)


def cost(flops):
    return pl.CostEstimate(flops=flops, bytes_accessed=1 << 20, transcendentals=0)


def params(mib):
    return pltpu.CompilerParams(vmem_limit_bytes=mib * 1024 * 1024)


def per_device(offsets, burgers, lines, pair_list, pair_count):
    blocks = offsets.shape[3]
    width = offsets.shape[5]
    sizes = tuple(lax.axis_size(a) for a in AXES)
    place = [lax.axis_index(a).astype(jnp.int32) for a in AXES]
    pos = jnp.stack(place)
    rows = pair_list.shape[0]
    for size in sizes:
        assert size & (size - 1) == 0
    own, bur, lin = (jnp.swapaxes(v[0, 0, 0], 0, 1) for v in (offsets, burgers, lines))
    cell_rows = 6 * blocks + 8
    slots = tuple(min(s, 3) for s in sizes)
    part = pltpu.VMEM(own.shape, jnp.float32)
    with jax.named_scope("packing"):
        cell, line = pl.pallas_call(
            functools.partial(pack_kernel, sizes, slots, blocks),
            out_shape=(
                jax.ShapeDtypeStruct((cell_rows, width), jnp.float32),
                jax.ShapeDtypeStruct((8, width), jnp.int32),
            ),
            in_specs=[VMEM] * 2 + [HBM] * 4,
            out_specs=(VMEM, VMEM),
            scratch_shapes=[
                pltpu.VMEM((LANES, LANES), jnp.float32),
                pltpu.VMEM((2, rows), jnp.int32), part, part, part,
                pltpu.SemaphoreType.DMA((4,)),
            ],
            compiler_params=params(4),
            name="pack",
        )(
            pos[None],
            pair_count[None],
            *[
                pltpu.with_memory_space_constraint(v, pltpu.HBM)
                for v in (pair_list.T, own, bur, lin)
            ],
        )
    with jax.named_scope("weights"):
        weights = pl.pallas_call(
            functools.partial(weight_kernel, blocks),
            out_shape=jax.ShapeDtypeStruct((blocks, 48, FORMS * LANES), jnp.bfloat16),
            in_specs=[VMEM],
            out_specs=VMEM,
            compiler_params=params(8),
            cost_estimate=cost(COST[3]),
            name="weight",
        )(cell)
    sums = jax.ShapeDtypeStruct((7 * blocks, 8, LANES), jnp.float32)

    def near(stage, sources, *others):
        total_cells = sum(s.shape[0] for s in sources)
        jobs = blocks + 2 * rows + total_cells * rows
        extra = [pltpu.VMEM(sums.shape, sums.dtype)] if stage == 2 else []
        with jax.named_scope("near%d" % stage):
            return pl.pallas_call(
                functools.partial(near_kernel, stage, slots, blocks, rows),
                out_shape=jax.ShapeDtypeStruct(own.shape, jnp.float32) if stage == 2 else sums,
                in_specs=[VMEM] * (3 + len(sources) + len(others)),
                out_specs=VMEM,
                scratch_shapes=extra
                + [
                    pltpu.SMEM((jobs,), jnp.int32),
                    pltpu.VMEM((-(-(total_cells + 2) // 8) * 8, LANES), jnp.int32),
                    pltpu.SMEM((-(-(total_cells + 2) // 8) * 8, LANES), jnp.int32),
                    pltpu.SemaphoreType.DMA,
                ]
                + [pltpu.VMEM((LANES, 48), jnp.bfloat16)] * WAYS,
                compiler_params=params(8),
                cost_estimate=cost(COST[stage]),
                name="near%d" % stage,
            )(pos[None], line, weights, *sources, *others)

    every = coupling_rows(*sizes)
    with jax.named_scope("couple"):
        table = pl.pallas_call(
            functools.partial(couple_kernel, sizes),
            out_shape=jax.ShapeDtypeStruct((math.prod(sizes), every.shape[1]), jnp.float32),
            in_specs=[SMEM, VMEM],
            out_specs=VMEM,
            compiler_params=params(16),
            cost_estimate=cost(COST[3]),
            name="couple",
        )(pos, jnp.asarray(every))
    at = 6 * blocks + 1
    level = cell[None]
    moments = level[:, at, :]
    near0 = near(0, [level])
    for axis in ("gy", "gz"):
        carried = moments.shape[0] == level.shape[0]
        with jax.named_scope("halo_" + axis):
            found = neighbours(level, axis)
        if axis == "gz" and found:
            found[-1], table = lax.optimization_barrier((found[-1], table))
        step = 1
        if carried and found:
            moments = joined(moments, found[0][:, at, :])
            step = 2
        while step < lax.axis_size(axis):
            moments = joined(moments, crossed(moments, axis, step))
            step *= 2
        level = jnp.concatenate([level] + found, axis=0)
    with jax.named_scope("halo_gx"):
        sides = neighbours(level, "gx")
    near1 = near(1, [level], near0)
    parts = [moments]
    step = 1
    while step < sizes[0]:
        got = crossed(moments, "gx", step)
        parts.append(got)
        step *= 2
        if step < sizes[0]:
            moments = joined(moments, got)
    keep, fold = sum_masks(every.shape[1])
    with jax.named_scope("local"):
        local = pl.pallas_call(
            local_kernel,
            out_shape=jax.ShapeDtypeStruct((8, LANES), jnp.float32),
            in_specs=[VMEM] * (3 + len(parts)),
            out_specs=VMEM,
            compiler_params=params(16),
            cost_estimate=cost(COST[3]),
            name="local",
        )(table, jnp.asarray(keep), jnp.asarray(fold, jnp.bfloat16), *parts)
    forces = near(2, sides, near1, cell, local)
    return jnp.swapaxes(forces, 0, 1)[None, None, None]


def solution(mesh):
    return jax.shard_map(
        per_device,
        mesh=mesh,
        in_specs=(
            P("gx", "gy", "gz", None, None, None),
            P("gx", "gy", "gz", None, None, None),
            P("gx", "gy", "gz", None, None, None),
            P(("gx", "gy", "gz"), None),
            P(("gx", "gy", "gz")),
        ),
        out_specs=P("gx", "gy", "gz", None, None, None),
        check_vma=False,
    )
```
